32 devices in a mesh: row: 4 (over z), col: 8 (over y, x, core).
Axes of the slice: x: 2, y: 2, z: 4, core: 2. Of those that a mesh axis runs over, the one named last changes fastest.
Arguments:
- fine_residual: bfloat16 [16, 524288], P(None, ('row', 'col')), may hold values from -6 to 6
- tiles_one: bfloat16 [8192, 128, 128], P(('row', 'col')), may hold values from -0.1875 to 0.1875
- pointers_one: int32 [4128], P(('row', 'col')), may hold values from 0 to 256, as said below
- columns_one: int32 [8192], P(('row', 'col')), may hold values from 0 to 1023, as said below
- points_one: int32 [131072], P(('col', 'row')), may hold values from 0 to 16383, as said below
- tiles_two: bfloat16 [4096, 128, 128], P(('row', 'col')), may hold values from -0.125 to 0.125
- pointers_two: int32 [2080], P(('row', 'col')), may hold values from 0 to 128, as said below
- columns_two: int32 [4096], P(('row', 'col')), may hold values from 0 to 127
- points_two: int32 [32768], P(('row', 'col')), may hold values from 0 to 4095, as said below
- tiles_three: bfloat16 [512, 128, 128], P(('row', 'col')), may hold values from -0.1875 to 0.1875
- pointers_three: int32 [288], P(('row', 'col')), may hold values from 0 to 16, as said below
- columns_three: int32 [512], P(('row', 'col')), may hold values from 0 to 63
- points_three: int32 [8192], P(('col', 'row')), may hold values from 0 to 1023, as said below
Outputs:
- coarse_one: bfloat16 [16, 131072], P(None, ('col', 'row'))
- coarse_two: bfloat16 [16, 32768], P(None, ('row', 'col'))
- coarse_three: bfloat16 [16, 8192], P(None, ('col', 'row'))
The draws below stay inside these ranges and needn't reach their ends.
Inputs may be any that keep to these rules, and one draw needn't show every extreme that they name: `pointers_one`: each tile set's 128 + 1 pointers start at 0 and never fall; the last is that set's live slot count, at most 256; some set has 256 live slots. `pointers_two`: each tile set's 64 + 1 pointers start at 0 and never fall; the last is that set's live slot count, at most 128; some set has 128 live slots. `pointers_three`: each tile set's 8 + 1 pointers start at 0 and never fall; the last is that set's live slot count, at most 16; some set has 16 live slots. `columns_one`: among the live slots of one tile set, at most 32 name block columns with the same quotient by 128; some set reaches 32. `points_one`: values are distinct within each aligned run of 4096 entries. `points_two`: values are distinct within each aligned run of 1024 entries. `points_three`: values are distinct within each aligned run of 256 entries.
All inputs are finite; a program needn't handle non-finite values.
Results may differ from the reference program's by a relative error of at most 0.0057.
Values may be sent and summed in bfloat16 or wider, within the bound.
A program may use at most 128 MiB of HBM per device.

```python
import jax
import jax.numpy as jnp
from jax import lax

TILE_EDGE = 128
VECTORS = 16
PIECE_ROWS = 16384
FINE_ROWS = 524288
COARSE_ONE = 131072
COARSE_TWO = 32768
COARSE_THREE = 8192
BLOCKS_ONE = 128
BLOCKS_TWO = 64
BLOCKS_THREE = 8
SLOTS_ONE = 256
SLOTS_TWO = 128
SLOTS_THREE = 16
FINE_BLOCKS_TWO = 128
FINE_BLOCKS_THREE = 64
PEER_SLOTS = 32
N_ROW = 4
N_COL = 8
DEVICES = 32


def live_counts(level_key, slot_count):
    shifts = jax.random.randint(jax.random.fold_in(level_key, 11), (DEVICES,), 0, 5)
    forced = jax.random.randint(jax.random.fold_in(level_key, 12), (), 0, DEVICES)
    shifts = jnp.where(jnp.arange(DEVICES) == forced, 0, shifts)
    full_slots = jnp.full((DEVICES,), slot_count, jnp.int32)
    return jnp.maximum(jnp.right_shift(full_slots, shifts.astype(jnp.int32)), 1).astype(jnp.int32)


def pointer_table(level_key, slot_count, block_count):
    counts = live_counts(level_key, slot_count)
    block_draw = jax.random.randint(jax.random.fold_in(level_key, 13), (DEVICES, slot_count), 0, block_count)
    positions = jnp.arange(slot_count, dtype=jnp.int32)
    block_draw = jnp.where(positions[None, :] < counts[:, None], block_draw, block_count)
    ordered = jnp.sort(block_draw, axis=1)
    bounds = jnp.arange(block_count + 1, dtype=jnp.int32)
    table = jnp.sum((ordered[:, None, :] < bounds[None, :, None]).astype(jnp.int32), axis=2)
    return table.reshape(-1).astype(jnp.int32)


def point_table(level_key, piece_in, piece_out):
    keys = jax.random.split(level_key, DEVICES)
    chosen = jax.vmap(lambda single: jax.random.permutation(single, piece_in)[:piece_out])(keys)
    return chosen.reshape(-1).astype(jnp.int32)


def draw_pointers_one(key, part):
    return pointer_table(jax.random.fold_in(key, 1), SLOTS_ONE, BLOCKS_ONE)


def draw_pointers_two(key, part):
    return pointer_table(jax.random.fold_in(key, 2), SLOTS_TWO, BLOCKS_TWO)


def draw_pointers_three(key, part):
    return pointer_table(jax.random.fold_in(key, 3), SLOTS_THREE, BLOCKS_THREE)


def draw_columns_one(key, part):
    level_key = jax.random.fold_in(key, 1)
    counts = live_counts(level_key, SLOTS_ONE)
    blocks_peer = PIECE_ROWS // TILE_EDGE
    positions = jnp.arange(SLOTS_ONE, dtype=jnp.int32)
    is_live = positions[None, :] < counts[:, None]
    scores = jax.random.randint(jax.random.fold_in(key, 21), (DEVICES, SLOTS_ONE), 0, 1 << 20) * SLOTS_ONE + positions[None, :]
    scores = jnp.where(is_live, scores, scores + (1 << 30))
    rank_order = jnp.argsort(scores, axis=1)
    hot_rank = jnp.argsort(rank_order, axis=1)
    hot_take = jnp.minimum(counts, PEER_SLOTS)
    is_hot = hot_rank < hot_take[:, None]
    hot_peer = jax.random.randint(jax.random.fold_in(key, 22), (DEVICES,), 0, N_COL)
    base_list = jnp.arange((N_COL - 1) * PEER_SLOTS, dtype=jnp.int32) % (N_COL - 1)
    other_keys = jax.random.split(jax.random.fold_in(key, 23), DEVICES)
    others = jax.vmap(lambda single: jax.random.permutation(single, base_list))(other_keys)
    other_rank = jnp.cumsum(1 - is_hot.astype(jnp.int32), axis=1) - 1
    other_rank = jnp.clip(other_rank, 0, (N_COL - 1) * PEER_SLOTS - 1)
    other_choice = jnp.take_along_axis(others, other_rank, axis=1)
    owner_peer = jnp.where(is_hot, hot_peer[:, None], (hot_peer[:, None] + 1 + other_choice) % N_COL)
    offsets = jax.random.randint(jax.random.fold_in(key, 24), (DEVICES, SLOTS_ONE), 0, blocks_peer)
    return (owner_peer * blocks_peer + offsets).reshape(-1).astype(jnp.int32)


def draw_points_one(key, part):
    return point_table(jax.random.fold_in(key, 31), PIECE_ROWS, PIECE_ROWS // 4)


def draw_points_two(key, part):
    return point_table(jax.random.fold_in(key, 32), PIECE_ROWS // 4, PIECE_ROWS // 16)


def draw_points_three(key, part):
    return point_table(jax.random.fold_in(key, 33), PIECE_ROWS // 16, PIECE_ROWS // 64)


def plant(result, own_key, least, largest):
    dims = result.shape
    spot = [jax.random.randint(jax.random.fold_in(own_key, axis), (), 0, dims[axis]) for axis in range(len(dims))]
    result = result.at[tuple(spot)].set(least)
    longest = dims.index(max(dims))
    spot[longest] = (spot[longest] + 1) % dims[longest]
    return result.at[tuple(spot)].set(largest)


def block_scale(rng, extent, cuts, low, high):
    def one(position, blocks):
        draws = jax.random.uniform(jax.random.fold_in(jax.random.fold_in(rng, 6), position), (blocks,), jnp.float32, low / len(cuts), high / len(cuts))
        return jnp.repeat(jnp.exp(draws), extent[position] // blocks).reshape((-1,) + (1,) * (len(extent) - position - 1))

    level = one(*cuts[0])
    for cut in cuts[1:]:
        level = level * one(*cut)
    return level


def gaussian(rng, shape, deviation, most, pieces=(), kind=jnp.bfloat16):
    array = jax.random.normal(rng, shape, jnp.float32) * deviation
    if len(pieces) > 0:
        array = block_scale(rng, shape, pieces, -0.22, 0.18) * array
    return jnp.clip(array, min=-most, max=most).astype(kind)


def setup_inputs(seed: int = 0) -> dict:
    arg_keys = jax.random.split(jax.random.key(seed), 14)
    return {
        "fine_residual": gaussian(arg_keys[0], (VECTORS, FINE_ROWS), 1.0, 6.0, ((1, 32),)),
        "tiles_one": gaussian(arg_keys[1], (DEVICES * SLOTS_ONE, TILE_EDGE, TILE_EDGE), (2 * TILE_EDGE * N_ROW) ** -0.5, 0.1875, ((0, 32),)),
        "pointers_one": draw_pointers_one(jax.random.fold_in(arg_keys[13], 71), 0),
        "columns_one": draw_columns_one(jax.random.fold_in(arg_keys[13], 71), 0),
        "points_one": draw_points_one(jax.random.fold_in(arg_keys[13], 71), 0),
        "tiles_two": gaussian(arg_keys[5], (DEVICES * SLOTS_TWO, TILE_EDGE, TILE_EDGE), (2 * TILE_EDGE * N_COL) ** -0.5, 0.125, ((0, 32),)),
        "pointers_two": draw_pointers_two(jax.random.fold_in(arg_keys[13], 71), 0),
        "columns_two": plant(jax.random.randint(arg_keys[7], (DEVICES * SLOTS_TWO,), 0, FINE_BLOCKS_TWO), jax.random.fold_in(arg_keys[7], 1), 0, FINE_BLOCKS_TWO - 1).astype(jnp.int32),
        "points_two": draw_points_two(jax.random.fold_in(arg_keys[13], 71), 0),
        "tiles_three": gaussian(arg_keys[9], (DEVICES * SLOTS_THREE, TILE_EDGE, TILE_EDGE), (2 * TILE_EDGE * N_ROW) ** -0.5, 0.1875, ((0, 32),)),
        "pointers_three": draw_pointers_three(jax.random.fold_in(arg_keys[13], 71), 0),
        "columns_three": plant(jax.random.randint(arg_keys[11], (DEVICES * SLOTS_THREE,), 0, FINE_BLOCKS_THREE), jax.random.fold_in(arg_keys[11], 1), 0, FINE_BLOCKS_THREE - 1).astype(jnp.int32),
        "points_three": draw_points_three(jax.random.fold_in(arg_keys[13], 71), 0),
    }


def level_tiles(vector, tiles, columns, pointers, slot_count, block_count, fine_size, coarse_size, coarse_total, even_level):
    tile_edge = tiles.shape[1]
    vector_count = vector.shape[0]
    positions = jnp.arange(slot_count, dtype=jnp.int32)

    def one_device(running, device):
        if even_level:
            fine_index = device // N_COL
            coarse_index = device % N_COL
        else:
            fine_index = device % N_COL
            coarse_index = device // N_COL
        my_tiles = lax.dynamic_slice_in_dim(tiles, (device * slot_count).astype(jnp.int32), slot_count, 0).astype(jnp.float32)
        my_columns = lax.dynamic_slice_in_dim(columns, (device * slot_count).astype(jnp.int32), slot_count, 0)
        my_pointers = lax.dynamic_slice_in_dim(pointers, (device * (block_count + 1)).astype(jnp.int32), block_count + 1, 0)
        is_live = positions < my_pointers[block_count]
        finished = jnp.sum((my_pointers[1:][None, :] <= positions[:, None]).astype(jnp.int32), axis=1)
        segment = jnp.where(is_live, finished, block_count).astype(jnp.int32)
        fine_group = lax.dynamic_slice_in_dim(vector, (fine_index * fine_size).astype(jnp.int32), fine_size, 1).astype(jnp.float32)
        blocks = fine_group.reshape(vector_count, fine_size // tile_edge, tile_edge)
        picked = jnp.take(blocks, my_columns, axis=1)
        products = jnp.einsum("sij,vsj->svi", my_tiles, picked, precision=lax.Precision.HIGHEST)
        summed = jax.ops.segment_sum(products, segment, num_segments=block_count + 1)[:block_count]
        part_sum = jnp.transpose(summed, (1, 0, 2)).reshape(vector_count, coarse_size)
        offset = (coarse_index * coarse_size).astype(jnp.int32)
        current = lax.dynamic_slice_in_dim(running, offset, coarse_size, 1)
        return lax.dynamic_update_slice_in_dim(running, current + part_sum, offset, 1), None

    initial = jnp.zeros((vector_count, coarse_total), jnp.float32)
    running, unused = lax.scan(one_device, initial, jnp.arange(DEVICES, dtype=jnp.int32))
    return running


def point_rows(points, piece_in, piece_out, even_level):
    piece_index = jnp.arange(points.shape[0], dtype=jnp.int32) // piece_out
    if even_level:
        grid_row = piece_index % N_ROW
        grid_col = piece_index // N_ROW
        source = grid_row * N_COL + grid_col
    else:
        grid_row = piece_index // N_COL
        grid_col = piece_index % N_COL
        source = grid_col * N_ROW + grid_row
    return (source * piece_in + points).astype(jnp.int32)


def restrict(vector, tiles, columns, pointers, points, slot_count, block_count, fine_size, coarse_size, coarse_total, piece_in, even_level):
    running = level_tiles(vector, tiles, columns, pointers, slot_count, block_count, fine_size, coarse_size, coarse_total, even_level)
    fine_point = point_rows(points, piece_in, coarse_total // DEVICES, even_level)
    injected = jnp.take(vector, fine_point, axis=1).astype(jnp.float32)
    return (running + injected).astype(jnp.bfloat16)


def reference(fine_residual, tiles_one, pointers_one, columns_one, points_one, tiles_two, pointers_two, columns_two, points_two, tiles_three, pointers_three, columns_three, points_three):
    coarse_one = restrict(fine_residual, tiles_one, columns_one, pointers_one, points_one, SLOTS_ONE, BLOCKS_ONE, FINE_ROWS // N_ROW, COARSE_ONE // N_COL, COARSE_ONE, PIECE_ROWS, True)
    coarse_two = restrict(coarse_one, tiles_two, columns_two, pointers_two, points_two, SLOTS_TWO, BLOCKS_TWO, COARSE_ONE // N_COL, COARSE_TWO // N_ROW, COARSE_TWO, PIECE_ROWS // 4, False)
    coarse_three = restrict(coarse_two, tiles_three, columns_three, pointers_three, points_three, SLOTS_THREE, BLOCKS_THREE, COARSE_TWO // N_ROW, COARSE_THREE // N_COL, COARSE_THREE, PIECE_ROWS // 16, True)
    return (coarse_one, coarse_two, coarse_three)
```

```python
import functools

import jax
import jax.numpy as jnp
from jax import lax
from jax.experimental import pallas as pl
from jax.experimental.pallas import tpu as pltpu
from jax.sharding import PartitionSpec as P

CHUNKS = 2
BATCH = 16


def mirrored(index, mask, count):
    flipped = index
    bit = 1
    while bit < count:
        if mask & bit:
            flipped = flipped + bit * (1 - 2 * lax.rem(index // bit, 2))
        bit *= 2
    return flipped


def mirror_order(count):
    return sorted(range(1, count), key=lambda mask: (bin(mask).count("1"), mask))


def shift_of(size):
    assert size & (size - 1) == 0
    return size.bit_length() - 1


def down(row):
    edge = 128
    parts = []
    for first in range(0, row.shape[1], edge):
        spread = jnp.broadcast_to(row[:, first : first + edge], (edge, edge))
        parts.append(jnp.transpose(spread, (1, 0)))
    return parts


def plan(columns_ref, live, peers, blocks_peer, requests_ref, slots_ref, targets_ref):
    slots = columns_ref.shape[1]
    edge = 128
    per_peer = slots // peers
    columns = columns_ref[...]
    places = lax.broadcasted_iota(jnp.int32, (1, slots), 1)
    owner = jnp.right_shift(columns, shift_of(blocks_peer))
    within = jnp.bitwise_and(columns, blocks_peer - 1)
    owner = jnp.where(places < live, owner, peers + places)
    rank = jnp.zeros((1, slots), jnp.int32)
    owners_down = down(owner)
    for part, other in enumerate(owners_down):
        lines = lax.broadcasted_iota(jnp.int32, (edge, edge), 0) + part * edge
        ranks = []
        for first in range(0, slots, edge):
            lanes = lax.broadcasted_iota(jnp.int32, (edge, edge), 1) + first
            here = jnp.broadcast_to(owner[:, first : first + edge], (edge, edge))
            same = jnp.where((other == here) & (lines < lanes), 1, 0)
            ranks.append(jnp.sum(same, axis=0, keepdims=True))
        rank = rank + jnp.concatenate(ranks, axis=1)
    target = jnp.where(places < live, owner * per_peer + rank, slots)
    targets_ref[...] = jnp.where(places < live, target, 0)
    targets_down = down(target)
    within_down = down(within)
    for first in range(0, slots, edge):
        lanes = lax.broadcasted_iota(jnp.int32, (edge, edge), 1) + first
        request = jnp.zeros((1, edge), jnp.int32)
        slot = jnp.zeros((1, edge), jnp.int32)
        for part in range(slots // edge):
            lines = lax.broadcasted_iota(jnp.int32, (edge, edge), 0) + part * edge
            hit = targets_down[part] == lanes
            request = request + jnp.sum(jnp.where(hit, within_down[part], 0), axis=0, keepdims=True)
            slot = slot + jnp.sum(jnp.where(hit, lines, 0), axis=0, keepdims=True)
        requests_ref[:, first : first + edge] = request
        slots_ref[:, first : first + edge] = slot


def pair_products(tiles, sources):
    none = jnp.zeros_like(sources[0])
    left = jnp.concatenate([sources[0], none], axis=1)
    right = jnp.concatenate([none, sources[1]], axis=1)
    both = lax.dot_general(
        jnp.concatenate([left, right], axis=0),
        jnp.concatenate(tiles, axis=1),
        (((1,), (1,)), ((), ())),
        preferred_element_type=jnp.float32,
    )
    vectors = sources[0].shape[0]
    return both[:vectors], both[vectors:]


def some_products(tiles_ref, number, tile_of, source_of):
    products = []
    for i in range(0, number, 2):
        products += pair_products(
            [tiles_ref[tile_of(i)], tiles_ref[tile_of(i + 1)]], [source_of(i), source_of(i + 1)]
        )
    return products


def points_groups(first, last, points_ref, block_of, blocks, span, out_ref):
    edge = out_ref.shape[2]
    vectors = out_ref.shape[1]
    wide = points_ref.shape[2]
    group = wide // edge

    def one_group(number, carry):
        points = points_ref[number]
        owners = jnp.broadcast_to(jnp.right_shift(points, shift_of(edge)), (vectors, wide))
        lanes = jnp.broadcast_to(jnp.bitwise_and(points, edge - 1), (edge, wide))
        spots = lax.broadcasted_iota(jnp.int32, (edge, wide), 0)
        pick = (lanes == spots).astype(jnp.float32).astype(jnp.bfloat16)
        found = jnp.zeros((vectors, wide), jnp.float32)
        for part in range(blocks // span):
            rows = jnp.concatenate([block_of(part * span + k) for k in range(span)], axis=0)
            moved = jnp.dot(rows, pick, preferred_element_type=jnp.float32)
            for k in range(span):
                here = moved[k * vectors : (k + 1) * vectors]
                found = jnp.where(owners == part * span + k, here, found)
        for i in range(group):
            out_ref[number * group + i] = found[:, i * edge : (i + 1) * edge]
        return carry

    lax.fori_loop(first, last, one_group, 0)


def kernel(
    axes,
    fine_ref,
    columns_ref,
    tiles_one,
    tiles_two,
    tiles_three,
    pointers_one,
    pointers_two,
    pointers_three,
    columns_two,
    columns_three,
    points_one,
    points_two,
    points_three,
    out_one,
    out_two,
    out_three,
    requests_v,
    slots_v,
    targets_v,
    asked_v,
    slots_s,
    targets_s,
    asked_s,
    fine_blocks,
    replies_out,
    replies,
    held_one,
    held_two,
    held_three,
    products_one,
    sums_one,
    sums_two,
    sums_three,
    partial_one,
    partial_two,
    partial_three,
    arrived_one,
    arrived_two,
    arrived_three,
    injected_one,
    injected_two,
    injected_three,
    group_one,
    group_two,
    local_sem,
    request_sem,
    reply_sem,
    sum_one_sem,
    own_one_sem,
    sum_two_sem,
    own_two_sem,
    sum_three_sem,
):
    rows, cols = axes
    row, col = lax.axis_index("row"), lax.axis_index("col")
    edge = held_one.shape[2]
    slots = columns_ref.shape[1]
    per_peer = slots // cols
    blocks_peer = fine_ref.shape[1] // edge
    row_peers = [(k, lax.rem(row + k, rows)) for k in range(1, rows)]
    col_peers = [(m, mirrored(col, m, cols)) for m in mirror_order(cols)]
    mesh_id = pl.DeviceIdType.MESH

    barrier = pltpu.get_barrier_semaphore()
    for _, peer in row_peers:
        pl.semaphore_signal(barrier, inc=1, device_id={"row": peer}, device_id_type=mesh_id)
    for _, peer in col_peers:
        pl.semaphore_signal(barrier, inc=1, device_id={"col": peer}, device_id_type=mesh_id)
    loads = [
        pltpu.make_async_copy(source, held, local_sem.at[i])
        for i, (source, held) in enumerate(
            [(tiles_one, held_one), (tiles_two, held_two), (tiles_three, held_three)]
        )
    ]
    for load in loads:
        load.start()

    for j in range(blocks_peer):
        fine_blocks[j] = fine_ref[:, j * edge : (j + 1) * edge]
    plan(columns_ref, pointers_one[pointers_one.shape[0] - 1], cols, blocks_peer, requests_v, slots_v, targets_v)
    plans = [
        pltpu.make_async_copy(requests_v, asked_s.at[0], local_sem.at[3]),
        pltpu.make_async_copy(slots_v, slots_s, local_sem.at[4]),
        pltpu.make_async_copy(targets_v, targets_s, local_sem.at[5]),
    ]
    for copy in plans:
        copy.start()
    pl.semaphore_wait(barrier, rows + cols - 2)

    def send(source, target, sems, at, device):
        copy = pltpu.make_async_remote_copy(
            src_ref=source,
            dst_ref=target,
            send_sem=sems.at[(0,) + at],
            recv_sem=sems.at[(1,) + at],
            device_id=device,
            device_id_type=mesh_id,
        )
        copy.start()
        return copy

    asks = [send(requests_v, asked_v.at[m - 1], request_sem, (m - 1,), {"col": peer}) for m, peer in col_peers]
    for copy in plans:
        copy.wait()

    def take(m, out_ref, place):
        base = col * per_peer

        def some(step, carry):
            for i in range(8):
                at = step * 8 + i
                out_ref[place, at] = fine_blocks[asked_s[m, 0, base + at]]
            return carry

        lax.fori_loop(0, per_peer // 8, some, 0)

    def products_of(m, owner):
        base = owner * per_peer
        batch = min(BATCH, per_peer)

        def some(step, carry):
            first = step * batch
            found = some_products(
                held_one,
                batch,
                lambda i: slots_s[0, base + first + i],
                lambda i: replies[m, first + i],
            )
            for i, product in enumerate(found):
                products_one[base + first + i] = product
            return carry

        lax.fori_loop(0, per_peer // batch, some, 0)

    groups = points_one.shape[0]
    span_one = min(blocks_peer, 32)

    def fine_static(j):
        return fine_blocks[j]

    def points_at_one(first, last):
        points_groups(first, last, points_one, fine_static, blocks_peer, span_one, injected_one)

    take(0, replies, 0)
    loads[0].wait()
    products_of(0, col)
    points_at_one(0, groups // 8)
    for copy in asks:
        copy.wait_recv()
    asked = pltpu.make_async_copy(asked_v, asked_s.at[pl.ds(1, cols - 1)], local_sem.at[6])
    asked.start()
    asked.wait()
    answers = []
    for m, peer in col_peers:
        take(m, replies_out, m - 1)
        answers.append(send(replies_out.at[m - 1], replies.at[m], reply_sem, (m - 1,), {"col": peer}))
    points_at_one(groups // 8, groups // 4)
    for (m, peer), copy in zip(col_peers, answers):
        copy.wait_recv()
        products_of(m, peer)

    def run_one(step, total):
        for i in range(8):
            at = step * 8 + i
            total = total + products_one[targets_s[0, at]]
            sums_one[at + 1] = total
        return total

    sums_one[0] = jnp.zeros(sums_one.shape[1:], jnp.float32)
    lax.fori_loop(0, slots // 8, run_one, jnp.zeros(sums_one.shape[1:], jnp.float32))

    def block_sum(sums, pointers, block):
        return sums[pointers[block + 1]] - sums[pointers[block]]

    def partials(sums, pointers, partial, piece, first, size):
        per_piece = partial.shape[1]
        step_size = min(size, 8)

        def some(step, carry):
            for i in range(step_size):
                at = first + step * step_size + i
                partial[piece, at] = block_sum(sums, pointers, piece * per_piece + at).astype(partial.dtype)
            return carry

        lax.fori_loop(0, size // step_size, some, 0)

    def exchange(sums, pointers, partial, arrived, injected, chunks, peers, axis, me, sems, inject, group, own_sems, out):
        size = partial.shape[1] // chunks
        parts = [pl.ds(h * size, size) for h in range(chunks)]
        first, again = [], []
        for h, part in enumerate(parts):
            started = []
            for k, peer in peers:
                partials(sums, pointers, partial, peer, h * size, size)
                started.append(
                    send(partial.at[peer, part], arrived.at[k - 1, part], sems, (h, k - 1), {axis: peer})
                )
            first.append(started)
        inject()
        for h, part in enumerate(parts):
            base = me * partial.shape[1] + h * size
            own = [
                block_sum(sums, pointers, base + i) + injected[h * size + i] for i in range(size)
            ]
            for (k, _), copy in zip(peers, first[h]):
                copy.wait_recv()
                for i in range(size):
                    own[i] = own[i] + arrived[k - 1, h * size + i].astype(jnp.float32)
            for i in range(size):
                value = own[i].astype(out.dtype)
                at = h * size + i
                out[:, at * edge : (at + 1) * edge] = value
                if group is not None:
                    group[me, at] = value
            if group is not None:
                for k, peer in peers:
                    again.append(
                        send(group.at[me, part], group.at[me, part], own_sems, (h, k - 1), {axis: peer})
                    )
        return [copy for started in first for copy in started], again

    def restrict(held, columns, group, sums):
        number = held.shape[0]
        batch = min(BATCH, number)
        per_piece = group.shape[1]

        def some(step, total):
            first = step * batch

            def source_of(i):
                column = columns[first + i]
                return group[jnp.right_shift(column, shift_of(per_piece)), jnp.bitwise_and(column, per_piece - 1)]

            found = some_products(held, batch, lambda i: first + i, source_of)
            for i, product in enumerate(found):
                total = total + product
                sums[first + i + 1] = total
            return total

        sums[0] = jnp.zeros(sums.shape[1:], jnp.float32)
        lax.fori_loop(0, number // batch, some, jnp.zeros(sums.shape[1:], jnp.float32))

    sent_one, own_one = exchange(
        sums_one, pointers_one, partial_one, arrived_one, injected_one, sum_one_sem.shape[1], row_peers, "row", row,
        sum_one_sem, lambda: points_at_one(groups // 4, groups), group_one, own_one_sem, out_one,
    )

    def own_block_one(j):
        return group_one[row, j]

    points_groups(
        0, points_two.shape[0], points_two, own_block_one, group_one.shape[1], min(group_one.shape[1], 32), injected_two
    )
    loads[1].wait()
    for copy in own_one:
        copy.wait_recv()
    restrict(held_two, columns_two, group_one, sums_two)
    sent_two, own_two = exchange(
        sums_two, pointers_two, partial_two, arrived_two, injected_two, sum_two_sem.shape[1], col_peers, "col", col,
        sum_two_sem, lambda: None, group_two, own_two_sem, out_two,
    )

    def own_block_two(j):
        return group_two[col, j]

    points_groups(
        0, points_three.shape[0], points_three, own_block_two, group_two.shape[1], group_two.shape[1], injected_three
    )
    loads[2].wait()
    for copy in own_two:
        copy.wait_recv()
    restrict(held_three, columns_three, group_two, sums_three)
    sent_three, _ = exchange(
        sums_three, pointers_three, partial_three, arrived_three, injected_three, sum_three_sem.shape[1], row_peers,
        "row", row, sum_three_sem, lambda: None, None, None, out_three,
    )
    for copy in asks + answers + sent_one + own_one + sent_two + own_two + sent_three:
        copy.wait_send()


def on_device(
    fine_residual,
    tiles_one,
    pointers_one,
    columns_one,
    points_one,
    tiles_two,
    pointers_two,
    columns_two,
    points_two,
    tiles_three,
    pointers_three,
    columns_three,
    points_three,
):
    vectors = fine_residual.shape[0]
    edge = tiles_one.shape[1]
    rows, cols = lax.axis_size("row"), lax.axis_size("col")
    slots = tiles_one.shape[0]
    per_peer = slots // cols
    low, wide = fine_residual.dtype, jnp.float32
    piece_one = (pointers_one.shape[0] - 1) // rows
    piece_two = (pointers_two.shape[0] - 1) // cols
    piece_three = (pointers_three.shape[0] - 1) // rows
    chunks = CHUNKS if piece_one % CHUNKS == 0 else 1

    def grouped(points):
        size = points.shape[0] // edge
        group = min(size, 2)
        return points.reshape(size // group, 1, group * edge)

    block = (vectors, edge)
    vmem = pl.BlockSpec(memory_space=pltpu.VMEM)
    smem = pl.BlockSpec(memory_space=pltpu.SMEM)
    hbm = pl.BlockSpec(memory_space=pl.ANY)
    dma = pltpu.SemaphoreType.DMA
    scratch = [
        pltpu.VMEM((1, slots), jnp.int32),
        pltpu.VMEM((1, slots), jnp.int32),
        pltpu.VMEM((1, slots), jnp.int32),
        pltpu.VMEM((cols - 1, 1, slots), jnp.int32),
        pltpu.SMEM((1, slots), jnp.int32),
        pltpu.SMEM((1, slots), jnp.int32),
        pltpu.SMEM((cols, 1, slots), jnp.int32),
        pltpu.VMEM((fine_residual.shape[1] // edge,) + block, low),
        pltpu.VMEM((cols - 1, per_peer) + block, low),
        pltpu.VMEM((cols, per_peer) + block, low),
        pltpu.VMEM(tiles_one.shape, low),
        pltpu.VMEM(tiles_two.shape, low),
        pltpu.VMEM(tiles_three.shape, low),
        pltpu.VMEM((slots,) + block, wide),
        pltpu.VMEM((slots + 1,) + block, wide),
        pltpu.VMEM((tiles_two.shape[0] + 1,) + block, wide),
        pltpu.VMEM((tiles_three.shape[0] + 1,) + block, wide),
        pltpu.VMEM((rows, piece_one) + block, low),
        pltpu.VMEM((cols, piece_two) + block, low),
        pltpu.VMEM((rows, piece_three) + block, low),
        pltpu.VMEM((rows - 1, piece_one) + block, low),
        pltpu.VMEM((cols - 1, piece_two) + block, low),
        pltpu.VMEM((rows - 1, piece_three) + block, low),
        pltpu.VMEM((piece_one,) + block, wide),
        pltpu.VMEM((piece_two,) + block, wide),
        pltpu.VMEM((piece_three,) + block, wide),
        pltpu.VMEM((rows, piece_one) + block, low),
        pltpu.VMEM((cols, piece_two) + block, low),
        dma((7,)),
        dma((2, cols - 1)),
        dma((2, cols - 1)),
        dma((2, chunks, rows - 1)),
        dma((2, chunks, rows - 1)),
        dma((2, 1, cols - 1)),
        dma((2, 1, cols - 1)),
        dma((2, 1, rows - 1)),
    ]
    return pl.pallas_call(
        functools.partial(kernel, (rows, cols)),
        in_specs=[vmem] * 2 + [hbm] * 3 + [smem] * 5 + [vmem] * 3,
        out_specs=[vmem] * 3,
        out_shape=[
            jax.ShapeDtypeStruct((vectors, piece * edge), low) for piece in (piece_one, piece_two, piece_three)
        ],
        scratch_shapes=scratch,
        compiler_params=pltpu.CompilerParams(collective_id=0, has_side_effects=True),
        name="restrict_all",
    )(
        fine_residual,
        columns_one.reshape(1, slots),
        tiles_one,
        tiles_two,
        tiles_three,
        pointers_one,
        pointers_two,
        pointers_three,
        columns_two,
        columns_three,
        grouped(points_one),
        grouped(points_two),
        grouped(points_three),
    )


def solution(mesh):
    placed = (
        P(None, ("row", "col")),
        P(("row", "col"), None, None),
        P(("row", "col")),
        P(("row", "col")),
        P(("col", "row")),
        P(("row", "col"), None, None),
        P(("row", "col")),
        P(("row", "col")),
        P(("row", "col")),
        P(("row", "col"), None, None),
        P(("row", "col")),
        P(("row", "col")),
        P(("col", "row")),
    )
    return jax.shard_map(
        on_device,
        mesh=mesh,
        in_specs=placed,
        out_specs=(P(None, ("col", "row")), P(None, ("row", "col")), P(None, ("col", "row"))),
        check_vma=False,
    )
```

```python
import functools

import jax
import jax.numpy as jnp
from jax import lax
from jax.experimental import pallas as pl
from jax.experimental.pallas import tpu as pltpu
from jax.sharding import PartitionSpec as P

CHUNKS = 2
BATCH = 16


def mirrored(index, mask, count):
    flipped = index
    bit = 1
    while bit < count:
        if mask & bit:
            flipped = flipped + bit * (1 - 2 * lax.rem(index // bit, 2))
        bit *= 2
    return flipped


def mirror_order(count):
    return sorted(range(1, count), key=lambda mask: (bin(mask).count("1"), mask))


def shift_of(size):
    assert size & (size - 1) == 0
    return size.bit_length() - 1


def down(row):
    edge = 128
    parts = []
    for first in range(0, row.shape[1], edge):
        spread = jnp.broadcast_to(row[:, first : first + edge], (edge, edge))
        parts.append(jnp.transpose(spread, (1, 0)))
    return parts


def plan(columns_ref, live, peers, blocks_peer, requests_ref, slots_ref, targets_ref):
    slots = columns_ref.shape[1]
    edge = 128
    per_peer = slots // peers
    columns = columns_ref[...]
    places = lax.broadcasted_iota(jnp.int32, (1, slots), 1)
    owner = jnp.right_shift(columns, shift_of(blocks_peer))
    within = jnp.bitwise_and(columns, blocks_peer - 1)
    owner = jnp.where(places < live, owner, peers + places)
    rank = jnp.zeros((1, slots), jnp.int32)
    owners_down = down(owner)
    for part, other in enumerate(owners_down):
        lines = lax.broadcasted_iota(jnp.int32, (edge, edge), 0) + part * edge
        ranks = []
        for first in range(0, slots, edge):
            lanes = lax.broadcasted_iota(jnp.int32, (edge, edge), 1) + first
            here = jnp.broadcast_to(owner[:, first : first + edge], (edge, edge))
            same = jnp.where((other == here) & (lines < lanes), 1, 0)
            ranks.append(jnp.sum(same, axis=0, keepdims=True))
        rank = rank + jnp.concatenate(ranks, axis=1)
    target = jnp.where(places < live, owner * per_peer + rank, slots)
    targets_ref[...] = jnp.where(places < live, target, 0)
    targets_down = down(target)
    within_down = down(within)
    for first in range(0, slots, edge):
        lanes = lax.broadcasted_iota(jnp.int32, (edge, edge), 1) + first
        request = jnp.zeros((1, edge), jnp.int32)
        slot = jnp.zeros((1, edge), jnp.int32)
        for part in range(slots // edge):
            lines = lax.broadcasted_iota(jnp.int32, (edge, edge), 0) + part * edge
            hit = targets_down[part] == lanes
            request = request + jnp.sum(jnp.where(hit, within_down[part], 0), axis=0, keepdims=True)
            slot = slot + jnp.sum(jnp.where(hit, lines, 0), axis=0, keepdims=True)
        requests_ref[:, first : first + edge] = request
        slots_ref[:, first : first + edge] = slot


def pair_products(tiles, sources):
    none = jnp.zeros_like(sources[0])
    left = jnp.concatenate([sources[0], none], axis=1)
    right = jnp.concatenate([none, sources[1]], axis=1)
    both = lax.dot_general(
        jnp.concatenate([left, right], axis=0),
        jnp.concatenate(tiles, axis=1),
        (((1,), (1,)), ((), ())),
        preferred_element_type=jnp.float32,
    )
    vectors = sources[0].shape[0]
    return both[:vectors], both[vectors:]


def some_products(tiles_ref, number, tile_of, source_of):
    products = []
    for i in range(0, number, 2):
        products += pair_products(
            [tiles_ref[tile_of(i)], tiles_ref[tile_of(i + 1)]], [source_of(i), source_of(i + 1)]
        )
    return products


def points_groups(first, last, points_ref, block_of, blocks, span, out_ref):
    edge = out_ref.shape[2]
    vectors = out_ref.shape[1]
    wide = points_ref.shape[2]
    group = wide // edge

    def one_group(number, carry):
        points = points_ref[number]
        owners = jnp.broadcast_to(jnp.right_shift(points, shift_of(edge)), (vectors, wide))
        lanes = jnp.broadcast_to(jnp.bitwise_and(points, edge - 1), (edge, wide))
        spots = lax.broadcasted_iota(jnp.int32, (edge, wide), 0)
        pick = (lanes == spots).astype(jnp.float32).astype(jnp.bfloat16)
        found = jnp.zeros((vectors, wide), jnp.float32)
        for part in range(blocks // span):
            rows = jnp.concatenate([block_of(part * span + k) for k in range(span)], axis=0)
            moved = jnp.dot(rows, pick, preferred_element_type=jnp.float32)
            for k in range(span):
                here = moved[k * vectors : (k + 1) * vectors]
                found = jnp.where(owners == part * span + k, here, found)
        for i in range(group):
            out_ref[number * group + i] = found[:, i * edge : (i + 1) * edge]
        return carry

    lax.fori_loop(first, last, one_group, 0)


def kernel(axes, *refs):
    rows, cols = axes
    (fine_h, columns_h, pointers_one_h, pointers_two_h, pointers_three_h, columns_two_h, columns_three_h) = refs[:7]
    (points_one_h, points_two_h, points_three_h, tiles_one, tiles_two, tiles_three) = refs[7:13]
    out_one, out_two, out_three = refs[13:16]
    (fine_ref, columns_ref, pointers_one, pointers_two, pointers_three, columns_two, columns_three) = refs[16:23]
    (points_one, points_two, points_three, held_one, held_two, held_three) = refs[23:29]
    (requests_v, slots_v, targets_v, asked_v, slots_s, targets_s, asked_s) = refs[29:36]
    (fine_blocks, replies_out, replies, products_one, sums_one, sums_two, sums_three) = refs[36:43]
    (partial_one, partial_two, partial_three, arrived_one, passing, arrived_two, arrived_three) = refs[43:50]
    (injected_one, injected_two, injected_three, group_one, group_two) = refs[50:55]
    (load_sem, local_sem, request_sem, reply_sem, sum_one_sem, pass_sem, own_one_sem, on_sem) = refs[55:63]
    (sum_two_sem, own_two_sem, sum_three_sem) = refs[63:]

    row, col = lax.axis_index("row"), lax.axis_index("col")
    edge = held_one.shape[2]
    slots = columns_ref.shape[1]
    per_peer = slots // cols
    blocks_peer = fine_ref.shape[1] // edge
    row_peers = [(k, lax.rem(row + k, rows)) for k in range(1, rows)]
    col_peers = [(m, mirrored(col, m, cols)) for m in mirror_order(cols)]
    mesh_id = pl.DeviceIdType.MESH

    barrier = pltpu.get_barrier_semaphore()
    for _, peer in row_peers:
        pl.semaphore_signal(barrier, inc=1, device_id={"row": peer}, device_id_type=mesh_id)
    for _, peer in col_peers:
        pl.semaphore_signal(barrier, inc=1, device_id={"col": peer}, device_id_type=mesh_id)
    pairs = [
        (columns_h, columns_ref),
        (pointers_one_h, pointers_one),
        (fine_h, fine_ref),
        (points_one_h, points_one),
        (tiles_one, held_one),
        (pointers_two_h, pointers_two),
        (pointers_three_h, pointers_three),
        (columns_two_h, columns_two),
        (columns_three_h, columns_three),
        (points_two_h, points_two),
        (points_three_h, points_three),
        (tiles_two, held_two),
        (tiles_three, held_three),
    ]
    loads = [
        pltpu.make_async_copy(source, held, load_sem.at[i]) for i, (source, held) in enumerate(pairs)
    ]
    for load in loads:
        load.start()

    with jax.named_scope("wait_plan"):
        loads[0].wait()
        loads[1].wait()
    with jax.named_scope("plan"):
        plan(
            columns_ref,
            pointers_one[pointers_one.shape[0] - 1],
            cols,
            blocks_peer,
            requests_v,
            slots_v,
            targets_v,
        )
    plans = [
        pltpu.make_async_copy(requests_v, asked_s.at[0], local_sem.at[0]),
        pltpu.make_async_copy(slots_v, slots_s, local_sem.at[1]),
        pltpu.make_async_copy(targets_v, targets_s, local_sem.at[2]),
    ]
    with jax.named_scope("barrier"):
        pl.semaphore_wait(barrier, rows + cols - 2)

    def copy_to(source, target, out_sem, in_sem, device):
        return pltpu.make_async_remote_copy(
            src_ref=source,
            dst_ref=target,
            send_sem=out_sem,
            recv_sem=in_sem,
            device_id=device,
            device_id_type=mesh_id,
        )

    def send(source, target, sems, at, device):
        copy = copy_to(source, target, sems.at[(0,) + at], sems.at[(1,) + at], device)
        copy.start()
        return copy

    asks = [send(requests_v, asked_v.at[m - 1], request_sem, (m - 1,), {"col": peer}) for m, peer in col_peers]
    for copy in plans:
        copy.start()

    def take(m, out_ref, place):
        base = col * per_peer

        def some(step, carry):
            for i in range(8):
                at = step * 8 + i
                out_ref[place, at] = fine_blocks[asked_s[m, 0, base + at]]
            return carry

        lax.fori_loop(0, per_peer // 8, some, 0)

    def products_of(m, owner):
        base = owner * per_peer
        batch = min(BATCH, per_peer)

        def some(step, carry):
            first = step * batch
            found = some_products(
                held_one,
                batch,
                lambda i: slots_s[0, base + first + i],
                lambda i: replies[m, first + i],
            )
            for i, product in enumerate(found):
                products_one[base + first + i] = product
            return carry

        lax.fori_loop(0, per_peer // batch, some, 0)

    groups = points_one.shape[0]
    span_one = min(blocks_peer, 32)
    marks = [groups * part // 16 for part in (0, 5, 9, 13, 16)]

    def points_at_one(part):
        with jax.named_scope("points_one"):
            points_groups(
                marks[part],
                marks[part + 1],
                points_one,
                lambda j: fine_blocks[j],
                blocks_peer,
                span_one,
                injected_one,
            )

    with jax.named_scope("wait_fine"):
        loads[2].wait()
        loads[3].wait()
    with jax.named_scope("blocks"):
        for j in range(blocks_peer):
            fine_blocks[j] = fine_ref[:, j * edge : (j + 1) * edge]
    points_at_one(0)
    with jax.named_scope("wait_ask"):
        for copy in asks:
            copy.wait_recv()
        asked = pltpu.make_async_copy(asked_v, asked_s.at[pl.ds(1, cols - 1)], local_sem.at[3])
        asked.start()
        for copy in plans:
            copy.wait()
        take(0, replies, 0)
        asked.wait()
    answers = []
    with jax.named_scope("answer"):
        for m, peer in col_peers:
            take(m, replies_out, m - 1)
            answers.append(send(replies_out.at[m - 1], replies.at[m], reply_sem, (m - 1,), {"col": peer}))
    with jax.named_scope("wait_tiles"):
        loads[4].wait()
    products_of(0, col)
    points_at_one(1)
    for number, ((m, peer), copy) in enumerate(zip(col_peers, answers)):
        with jax.named_scope(f"wait_reply#m={m}"):
            copy.wait_recv()
        with jax.named_scope(f"products#m={m}"):
            products_of(m, peer)
        if number + 2 < len(marks) - 1:
            points_at_one(number + 2)
    for load in loads[5:]:
        load.wait()

    def run_one(step, total):
        for i in range(8):
            at = step * 8 + i
            total = total + products_one[targets_s[0, at]]
            sums_one[at + 1] = total
        return total

    with jax.named_scope("run_one"):
        sums_one[0] = jnp.zeros(sums_one.shape[1:], jnp.float32)
        lax.fori_loop(0, slots // 8, run_one, jnp.zeros(sums_one.shape[1:], jnp.float32))

    def block_sum(sums, pointers, block):
        return sums[pointers[block + 1]] - sums[pointers[block]]

    def partials(sums, pointers, partial, piece, first, size, more=None):
        per_piece = partial.shape[1]
        step_size = min(size, 8)

        def some(step, carry):
            for i in range(step_size):
                at = first + step * step_size + i
                total = block_sum(sums, pointers, piece * per_piece + at)
                if more is not None:
                    total = total + more[at].astype(jnp.float32)
                partial[piece, at] = total.astype(partial.dtype)
            return carry

        lax.fori_loop(0, size // step_size, some, 0)

    def along(first, last):
        for far in range(first, last, 1 if last > first else -1):
            for sign in (1, -1):
                other = row + sign * far
                yield far, sign, (other >= 0) & (other < rows), other

    end = rows - 1
    chunks = sum_one_sem.shape[1]
    size = partial_one.shape[1] // chunks
    parts = [pl.ds(h * size, size) for h in range(chunks)]
    waits = []

    def sum_copy(h, other):
        return copy_to(
            partial_one.at[other, parts[h]],
            arrived_one.at[row, parts[h]],
            sum_one_sem.at[0, h, other],
            sum_one_sem.at[1, h, row],
            {"row": other},
        )

    def sum_wait(h, other):
        return copy_to(
            partial_one.at[other, parts[h]],
            arrived_one.at[other, parts[h]],
            sum_one_sem.at[0, h, other],
            sum_one_sem.at[1, h, other],
            {"row": other},
        )

    def pass_copy(h, side, other, through):
        return copy_to(
            partial_one.at[other, parts[h]],
            passing.at[side, parts[h]],
            pass_sem.at[0, side, h],
            pass_sem.at[1, side, h],
            {"row": through},
        )

    sides = [(0, 0, 1, end), (1, end, end - 1, 0)]
    for h in range(chunks):
        with jax.named_scope(f"partials#h={h}"):
            for side, source, through, to in sides:

                @pl.when(row == source)
                def _():
                    partials(sums_one, pointers_one, partial_one, to, h * size, size)
                    pass_copy(h, side, to, through).start()

            for far, sign, valid, other in along(end - 1, 0):
                direct = valid
                if far == end - 1:
                    to = end if sign > 0 else 0
                    direct = valid & (other != to)

                @pl.when(direct)
                def _():
                    partials(sums_one, pointers_one, partial_one, other, h * size, size)
                    sum_copy(h, other).start()

    def pass_on(h):
        for side, source, through, to in sides:

            @pl.when(row == through)
            def _():
                pass_copy(h, side, to, through).wait_recv()
                partials(sums_one, pointers_one, partial_one, to, h * size, size, passing.at[side])
                sum_copy(h, to).start()

    def own_copy(h, piece, other, out_sem):
        return copy_to(
            group_one.at[piece, parts[h]],
            group_one.at[piece, parts[h]],
            out_sem,
            own_one_sem.at[1, h, piece],
            {"row": other},
        )

    def own_direct(far, other):
        if far == 1:
            return True
        return (other != 0) & (other != end)

    for h in range(chunks):
        with jax.named_scope(f"pass#h={h}"):
            pass_on(h)
        for far, sign, valid, other in along(1, rows):
            if far == end:
                continue

            @pl.when(valid)
            def _():
                with jax.named_scope(f"wait_sum#h={h}#far={far}"):
                    sum_wait(h, other).wait_recv()

        with jax.named_scope(f"own#h={h}"):
            base = row * partial_one.shape[1]

            def finish(i):
                at = h * size + i
                total = block_sum(sums_one, pointers_one, base + at) + injected_one[at]
                for other in range(rows):
                    comes = (row != other) & ((row - other) * (row - other) < end * end)
                    here = arrived_one[other, at].astype(jnp.float32)
                    total = total + jnp.where(comes, here, 0.0)
                value = total.astype(out_one.dtype)
                out_one[:, at * edge : (at + 1) * edge] = value
                group_one[row, at] = value

            for i in range(size):
                finish(i)
            for far, sign, valid, other in along(end, 0):

                @pl.when(valid & own_direct(far, other))
                def _():
                    own_copy(h, row, other, own_one_sem.at[0, h, other]).start()

    def points_at_two(first, last):
        with jax.named_scope("points_two"):
            points_groups(
                first,
                last,
                points_two,
                lambda j: group_one[row, j],
                group_one.shape[1],
                min(group_one.shape[1], 32),
                injected_two,
            )

    groups_two = points_two.shape[0]
    for h in range(chunks):
        for far in range(1, rows):
            for sign in (1, -1):
                other = row + sign * far
                valid = (other >= 0) & (other < rows)
                with jax.named_scope(f"wait_own#h={h}#far={far}"):

                    @pl.when(valid)
                    def _():
                        own_copy(h, other, row, own_one_sem.at[0, h, other]).wait_recv()

                    for to, through in ((end, end - 1), (0, 1)):

                        @pl.when(valid & (row == through) & ((other - to) * (other - to) > 1) & (other != to))
                        def _():
                            own_copy(h, other, to, on_sem.at[h, other]).start()

            if h == 0:
                points_at_two(groups_two * (far - 1) // end, groups_two * far // end)

    def drain_one():
        for h in range(chunks):
            for side, source, through, to in sides:

                @pl.when(row == source)
                def _():
                    pass_copy(h, side, to, through).wait_send()

                @pl.when(row == through)
                def _():
                    sum_copy(h, to).wait_send()

            for far, sign, valid, other in along(end - 1, 0):
                direct = valid
                if far == end - 1:
                    to = end if sign > 0 else 0
                    direct = valid & (other != to)

                @pl.when(direct)
                def _():
                    sum_copy(h, other).wait_send()

            for far, sign, valid, other in along(end, 0):

                @pl.when(valid & own_direct(far, other))
                def _():
                    own_copy(h, row, other, own_one_sem.at[0, h, other]).wait_send()

                for to, through in ((end, end - 1), (0, 1)):

                    @pl.when(valid & (row == through) & ((other - to) * (other - to) > 1) & (other != to))
                    def _():
                        own_copy(h, other, to, on_sem.at[h, other]).wait_send()

    def exchange(sums, pointers, partial, arrived, injected, peers, axis, me, sems, group, own_sems, out):
        size = partial.shape[1]
        first, again = [], []
        with jax.named_scope("partials"):
            for k, peer in peers:
                partials(sums, pointers, partial, peer, 0, size)
                first.append(send(partial.at[peer], arrived.at[k - 1], sems, (k - 1,), {axis: peer}))
        own = [block_sum(sums, pointers, me * size + i) + injected[i] for i in range(size)]
        for (k, _), copy in zip(peers, first):
            with jax.named_scope(f"wait_sum#k={k}"):
                copy.wait_recv()
            for i in range(size):
                own[i] = own[i] + arrived[k - 1, i].astype(jnp.float32)
        for i in range(size):
            value = own[i].astype(out.dtype)
            out[:, i * edge : (i + 1) * edge] = value
            if group is not None:
                group[me, i] = value
        if group is not None:
            for k, peer in peers:
                again.append(send(group.at[me], group.at[me], own_sems, (k - 1,), {axis: peer}))
        return first, again

    def restrict(held, columns, group, sums):
        number = held.shape[0]
        batch = min(2 * BATCH, number)
        per_piece = group.shape[1]

        def some(step, total):
            first = step * batch

            def source_of(i):
                column = columns[first + i]
                return group[jnp.right_shift(column, shift_of(per_piece)), jnp.bitwise_and(column, per_piece - 1)]

            found = some_products(held, batch, lambda i: first + i, source_of)
            for i, product in enumerate(found):
                total = total + product
                sums[first + i + 1] = total
            return total

        sums[0] = jnp.zeros(sums.shape[1:], jnp.float32)
        lax.fori_loop(0, number // batch, some, jnp.zeros(sums.shape[1:], jnp.float32))

    with jax.named_scope("restrict_two"):
        restrict(held_two, columns_two, group_one, sums_two)
    sent_two, own_two = exchange(
        sums_two, pointers_two, partial_two, arrived_two, injected_two, col_peers, "col", col, sum_two_sem, group_two,
        own_two_sem, out_two,
    )
    with jax.named_scope("points_three"):
        points_groups(
            0,
            points_three.shape[0],
            points_three,
            lambda j: group_two[col, j],
            group_two.shape[1],
            group_two.shape[1],
            injected_three,
        )
    with jax.named_scope("wait_group_two"):
        for copy in own_two:
            copy.wait_recv()
    with jax.named_scope("restrict_three"):
        restrict(held_three, columns_three, group_two, sums_three)
    sent_three, _ = exchange(
        sums_three, pointers_three, partial_three, arrived_three, injected_three, row_peers, "row", row, sum_three_sem,
        None, None, out_three,
    )
    with jax.named_scope("drain"):
        for copy in asks + answers + sent_two + own_two + sent_three:
            copy.wait_send()
        drain_one()


def tail_kernel(*refs):
    half = len(refs) // 2
    for source, out in zip(refs[:half], refs[half:]):
        out[...] = source[...]


def on_device(
    fine_residual,
    tiles_one,
    pointers_one,
    columns_one,
    points_one,
    tiles_two,
    pointers_two,
    columns_two,
    points_two,
    tiles_three,
    pointers_three,
    columns_three,
    points_three,
):
    vectors = fine_residual.shape[0]
    edge = tiles_one.shape[1]
    rows, cols = lax.axis_size("row"), lax.axis_size("col")
    slots = tiles_one.shape[0]
    per_peer = slots // cols
    low, wide = fine_residual.dtype, jnp.float32
    piece_one = (pointers_one.shape[0] - 1) // rows
    piece_two = (pointers_two.shape[0] - 1) // cols
    piece_three = (pointers_three.shape[0] - 1) // rows
    chunks = CHUNKS if piece_one % CHUNKS == 0 else 1

    def grouped(points):
        size = points.shape[0] // edge
        group = min(size, 2)
        return points.reshape(size // group, 1, group * edge)

    block = (vectors, edge)
    dma = pltpu.SemaphoreType.DMA
    inputs = [
        (fine_residual, pltpu.VMEM),
        (columns_one.reshape(1, slots), pltpu.VMEM),
        (pointers_one, pltpu.SMEM),
        (pointers_two, pltpu.SMEM),
        (pointers_three, pltpu.SMEM),
        (columns_two, pltpu.SMEM),
        (columns_three, pltpu.SMEM),
        (grouped(points_one), pltpu.VMEM),
        (grouped(points_two), pltpu.VMEM),
        (grouped(points_three), pltpu.VMEM),
        (tiles_one, pltpu.VMEM),
        (tiles_two, pltpu.VMEM),
        (tiles_three, pltpu.VMEM),
    ]
    scratch = [space(array.shape, array.dtype) for array, space in inputs]
    scratch += [
        pltpu.VMEM((1, slots), jnp.int32),
        pltpu.VMEM((1, slots), jnp.int32),
        pltpu.VMEM((1, slots), jnp.int32),
        pltpu.VMEM((cols - 1, 1, slots), jnp.int32),
        pltpu.SMEM((1, slots), jnp.int32),
        pltpu.SMEM((1, slots), jnp.int32),
        pltpu.SMEM((cols, 1, slots), jnp.int32),
        pltpu.VMEM((fine_residual.shape[1] // edge,) + block, low),
        pltpu.VMEM((cols - 1, per_peer) + block, low),
        pltpu.VMEM((cols, per_peer) + block, low),
        pltpu.VMEM((slots,) + block, wide),
        pltpu.VMEM((slots + 1,) + block, wide),
        pltpu.VMEM((tiles_two.shape[0] + 1,) + block, wide),
        pltpu.VMEM((tiles_three.shape[0] + 1,) + block, wide),
        pltpu.VMEM((rows, piece_one) + block, low),
        pltpu.VMEM((cols, piece_two) + block, low),
        pltpu.VMEM((rows, piece_three) + block, low),
        pltpu.VMEM((rows, piece_one) + block, low),
        pltpu.VMEM((2, piece_one) + block, low),
        pltpu.VMEM((cols - 1, piece_two) + block, low),
        pltpu.VMEM((rows - 1, piece_three) + block, low),
        pltpu.VMEM((piece_one,) + block, wide),
        pltpu.VMEM((piece_two,) + block, wide),
        pltpu.VMEM((piece_three,) + block, wide),
        pltpu.VMEM((rows, piece_one) + block, low),
        pltpu.VMEM((cols, piece_two) + block, low),
        dma((len(inputs),)),
        dma((4,)),
        dma((2, cols - 1)),
        dma((2, cols - 1)),
        dma((2, chunks, rows)),
        dma((2, 2, chunks)),
        dma((2, chunks, rows)),
        dma((chunks, rows)),
        dma((2, cols - 1)),
        dma((2, cols - 1)),
        dma((2, rows - 1)),
    ]
    shapes = [jax.ShapeDtypeStruct((vectors, piece * edge), low) for piece in (piece_one, piece_two, piece_three)]
    vmem = [pl.BlockSpec(memory_space=pltpu.VMEM)] * 3
    found = pl.pallas_call(
        functools.partial(kernel, (rows, cols)),
        in_specs=[pl.BlockSpec(memory_space=pl.ANY)] * len(inputs),
        out_specs=vmem,
        out_shape=shapes,
        scratch_shapes=scratch,
        compiler_params=pltpu.CompilerParams(
            collective_id=0, has_side_effects=True
        ),
        name="restrict_all",
    )(*[array for array, _ in inputs])
    return pl.pallas_call(
        tail_kernel,
        in_specs=vmem,
        out_specs=vmem,
        out_shape=shapes,
        name="results",
    )(*found)


def solution(mesh):
    placed = (
        P(None, ("row", "col")),
        P(("row", "col"), None, None),
        P(("row", "col")),
        P(("row", "col")),
        P(("col", "row")),
        P(("row", "col"), None, None),
        P(("row", "col")),
        P(("row", "col")),
        P(("row", "col")),
        P(("row", "col"), None, None),
        P(("row", "col")),
        P(("row", "col")),
        P(("col", "row")),
    )
    return jax.shard_map(
        on_device,
        mesh=mesh,
        in_specs=placed,
        out_specs=(P(None, ("col", "row")), P(None, ("row", "col")), P(None, ("col", "row"))),
        check_vma=False,
    )
```

```python
import functools

import jax
import jax.numpy as jnp
from jax import lax
from jax.experimental import pallas as pl
from jax.experimental.pallas import tpu as pltpu
from jax.sharding import PartitionSpec as P

SPLIT = (1, 1, 1, 1)
BATCH = 16


def mirrored(index, mask, count):
    flipped = index
    bit = 1
    while bit < count:
        if mask & bit:
            flipped = flipped + bit * (1 - 2 * lax.rem(index // bit, 2))
        bit *= 2
    return flipped


def mirror_order(count):
    return sorted(range(1, count), key=lambda mask: (bin(mask).count("1"), mask))


def far_order(count):
    return sorted(range(1, count), key=lambda mask: (-bin(mask >> 1).count("1"), mask & 1, mask))


def shift_of(size):
    assert size & (size - 1) == 0
    return size.bit_length() - 1


def down(row):
    edge = 128
    parts = []
    for first in range(0, row.shape[1], edge):
        spread = jnp.broadcast_to(row[:, first : first + edge], (edge, edge))
        parts.append(jnp.transpose(spread, (1, 0)))
    return parts


def plan(columns_ref, live, peers, blocks_peer, requests_ref, slots_ref, targets_ref):
    slots = columns_ref.shape[1]
    edge = 128
    per_peer = slots // peers
    columns = columns_ref[...]
    places = lax.broadcasted_iota(jnp.int32, (1, slots), 1)
    owner = jnp.right_shift(columns, shift_of(blocks_peer))
    within = jnp.bitwise_and(columns, blocks_peer - 1)
    owner = jnp.where(places < live, owner, peers + places)
    rank = jnp.zeros((1, slots), jnp.int32)
    owners_down = down(owner)
    for part, other in enumerate(owners_down):
        lines = lax.broadcasted_iota(jnp.int32, (edge, edge), 0) + part * edge
        ranks = []
        for first in range(0, slots, edge):
            lanes = lax.broadcasted_iota(jnp.int32, (edge, edge), 1) + first
            here = jnp.broadcast_to(owner[:, first : first + edge], (edge, edge))
            same = jnp.where((other == here) & (lines < lanes), 1, 0)
            ranks.append(jnp.sum(same, axis=0, keepdims=True))
        rank = rank + jnp.concatenate(ranks, axis=1)
    target = jnp.where(places < live, owner * per_peer + rank, slots)
    targets_ref[...] = jnp.where(places < live, target, 0)
    targets_down = down(target)
    within_down = down(within)
    for first in range(0, slots, edge):
        lanes = lax.broadcasted_iota(jnp.int32, (edge, edge), 1) + first
        request = jnp.zeros((1, edge), jnp.int32)
        slot = jnp.zeros((1, edge), jnp.int32)
        for part in range(slots // edge):
            lines = lax.broadcasted_iota(jnp.int32, (edge, edge), 0) + part * edge
            hit = targets_down[part] == lanes
            request = request + jnp.sum(jnp.where(hit, within_down[part], 0), axis=0, keepdims=True)
            slot = slot + jnp.sum(jnp.where(hit, lines, 0), axis=0, keepdims=True)
        requests_ref[:, first : first + edge] = request
        slots_ref[:, first : first + edge] = slot


def pair_products(tiles, sources):
    none = jnp.zeros_like(sources[0])
    left = jnp.concatenate([sources[0], none], axis=1)
    right = jnp.concatenate([none, sources[1]], axis=1)
    both = lax.dot_general(
        jnp.concatenate([left, right], axis=0),
        jnp.concatenate(tiles, axis=1),
        (((1,), (1,)), ((), ())),
        preferred_element_type=jnp.float32,
    )
    vectors = sources[0].shape[0]
    return both[:vectors], both[vectors:]


def some_products(tiles_ref, number, tile_of, source_of):
    products = []
    for i in range(0, number, 2):
        products += pair_products(
            [tiles_ref[tile_of(i)], tiles_ref[tile_of(i + 1)]], [source_of(i), source_of(i + 1)]
        )
    return products


def points_groups(first, last, points_ref, block_of, blocks, span, out_ref):
    edge = out_ref.shape[2]
    vectors = out_ref.shape[1]
    wide = points_ref.shape[2]
    group = wide // edge

    def one_group(number, carry):
        points = points_ref[number]
        owners = jnp.broadcast_to(jnp.right_shift(points, shift_of(edge)), (vectors, wide))
        lanes = jnp.broadcast_to(jnp.bitwise_and(points, edge - 1), (edge, wide))
        spots = lax.broadcasted_iota(jnp.int32, (edge, wide), 0)
        pick = (lanes == spots).astype(jnp.float32).astype(jnp.bfloat16)
        found = jnp.zeros((vectors, wide), jnp.float32)
        for part in range(blocks // span):
            rows = jnp.concatenate([block_of(part * span + k) for k in range(span)], axis=0)
            moved = jnp.dot(rows, pick, preferred_element_type=jnp.float32)
            for k in range(span):
                here = moved[k * vectors : (k + 1) * vectors]
                found = jnp.where(owners == part * span + k, here, found)
        for i in range(group):
            out_ref[number * group + i] = found[:, i * edge : (i + 1) * edge]
        return carry

    lax.fori_loop(first, last, one_group, 0)


def kernel(axes, *refs):
    rows, cols = axes
    (fine_h, columns_h, pointers_one_h, pointers_two_h, pointers_three_h, columns_two_h, columns_three_h) = refs[:7]
    (points_one_h, points_two_h, points_three_h, tiles_one, tiles_two, tiles_three) = refs[7:13]
    out_one, out_two, out_three = refs[13:16]
    (fine_ref, columns_ref, pointers_one, pointers_two, pointers_three, columns_two, columns_three) = refs[16:23]
    (points_one, points_two, points_three, held_one, held_two, held_three) = refs[23:29]
    (requests_v, slots_v, targets_v, slots_s, targets_s, asked_s) = refs[29:35]
    (fine_blocks, replies_out, replies, products_one, sums_one, sums_two, sums_three) = refs[35:42]
    (partial_one, partial_two, partial_three, arrived_one, passing, arrived_two, arrived_three) = refs[42:49]
    (injected_one, injected_two, injected_three, group_one, group_two) = refs[49:54]
    (load_sem, local_sem, request_sem, reply_sem, sum_one_sem, pass_sem, own_one_sem, on_sem) = refs[54:62]
    (sum_two_sem, own_two_sem, sum_three_sem) = refs[62:]

    row, col = lax.axis_index("row"), lax.axis_index("col")
    edge = held_one.shape[2]
    slots = columns_ref.shape[1]
    per_peer = slots // cols
    blocks_peer = fine_ref.shape[1] // edge
    row_peers = [(k, lax.rem(row + k, rows)) for k in range(1, rows)]
    col_peers = [(m, mirrored(col, m, cols)) for m in mirror_order(cols)]
    far_peers = [(m, mirrored(col, m, cols)) for m in far_order(cols)]
    mesh_id = pl.DeviceIdType.MESH

    barrier = pltpu.get_barrier_semaphore()
    for _, peer in row_peers:
        pl.semaphore_signal(barrier, inc=1, device_id={"row": peer}, device_id_type=mesh_id)
    for _, peer in col_peers:
        pl.semaphore_signal(barrier, inc=1, device_id={"col": peer}, device_id_type=mesh_id)
    pairs = [
        (columns_h, columns_ref),
        (pointers_one_h, pointers_one),
        (fine_h, fine_ref),
        (points_one_h, points_one),
        (tiles_one, held_one),
        (pointers_two_h, pointers_two),
        (pointers_three_h, pointers_three),
        (columns_two_h, columns_two),
        (columns_three_h, columns_three),
        (points_two_h, points_two),
        (points_three_h, points_three),
        (tiles_two, held_two),
        (tiles_three, held_three),
    ]
    loads = [
        pltpu.make_async_copy(source, held, load_sem.at[i]) for i, (source, held) in enumerate(pairs)
    ]
    for load in loads:
        load.start()

    with jax.named_scope("wait_plan"):
        loads[0].wait()
        loads[1].wait()
    with jax.named_scope("plan"):
        plan(
            columns_ref,
            pointers_one[pointers_one.shape[0] - 1],
            cols,
            blocks_peer,
            requests_v,
            slots_v,
            targets_v,
        )
    plans = [
        pltpu.make_async_copy(requests_v, asked_s.at[0], local_sem.at[0]),
        pltpu.make_async_copy(slots_v, slots_s, local_sem.at[1]),
        pltpu.make_async_copy(targets_v, targets_s, local_sem.at[2]),
    ]
    with jax.named_scope("barrier"):
        pl.semaphore_wait(barrier, rows + cols - 2)

    def copy_to(source, target, out_sem, in_sem, device):
        return pltpu.make_async_remote_copy(
            src_ref=source,
            dst_ref=target,
            send_sem=out_sem,
            recv_sem=in_sem,
            device_id=device,
            device_id_type=mesh_id,
        )

    def send(source, target, sems, at, device):
        copy = copy_to(source, target, sems.at[(0,) + at], sems.at[(1,) + at], device)
        copy.start()
        return copy

    asks = [send(requests_v, asked_s.at[m], request_sem, (m - 1,), {"col": peer}) for m, peer in col_peers]
    for copy in plans:
        copy.start()

    def take(m, out_ref, place):
        base = col * per_peer

        def some(step, carry):
            for i in range(8):
                at = step * 8 + i
                out_ref[place, at] = fine_blocks[asked_s[m, 0, base + at]]
            return carry

        lax.fori_loop(0, per_peer // 8, some, 0)

    def products_of(m, owner):
        base = owner * per_peer
        batch = min(BATCH, per_peer)

        def some(step, carry):
            first = step * batch
            found = some_products(
                held_one,
                batch,
                lambda i: slots_s[0, base + first + i],
                lambda i: replies[m, first + i],
            )
            for i, product in enumerate(found):
                products_one[base + first + i] = product
            return carry

        lax.fori_loop(0, per_peer // batch, some, 0)

    groups = points_one.shape[0]
    span_one = min(blocks_peer, 32)
    marks = [groups * part // 16 for part in (0, 5, 9, 13, 16)]

    def points_at_one(part):
        with jax.named_scope("points_one"):
            points_groups(
                marks[part],
                marks[part + 1],
                points_one,
                lambda j: fine_blocks[j],
                blocks_peer,
                span_one,
                injected_one,
            )

    with jax.named_scope("wait_fine"):
        loads[2].wait()
        loads[3].wait()
    with jax.named_scope("blocks"):
        for j in range(blocks_peer):
            fine_blocks[j] = fine_ref[:, j * edge : (j + 1) * edge]
    points_at_one(0)
    with jax.named_scope("wait_ask"):
        for copy in asks:
            copy.wait_recv()
        for copy in plans:
            copy.wait()
        take(0, replies, 0)
    answers = []
    with jax.named_scope("answer"):
        for m, peer in col_peers:
            take(m, replies_out, m - 1)
            answers.append(send(replies_out.at[m - 1], replies.at[m], reply_sem, (m - 1,), {"col": peer}))
    with jax.named_scope("wait_tiles"):
        loads[4].wait()
    products_of(0, col)
    points_at_one(1)
    coming = list(zip(col_peers, answers))
    for number, ((m, peer), copy) in enumerate(coming):
        with jax.named_scope(f"wait_reply#m={m}"):
            copy.wait_recv()
        with jax.named_scope(f"products#m={m}"):
            products_of(m, peer)
        if number + 2 < len(marks) - 1:
            points_at_one(number + 2)
    for load in loads[5:]:
        load.wait()

    def run_one(step, total):
        for i in range(8):
            at = step * 8 + i
            total = total + products_one[targets_s[0, at]]
            sums_one[at + 1] = total
        return total

    with jax.named_scope("run_one"):
        sums_one[0] = jnp.zeros(sums_one.shape[1:], jnp.float32)
        lax.fori_loop(0, slots // 8, run_one, jnp.zeros(sums_one.shape[1:], jnp.float32))

    def block_sum(sums, pointers, block):
        return sums[pointers[block + 1]] - sums[pointers[block]]

    def partials(sums, pointers, partial, piece, first, size, more=None):
        per_piece = partial.shape[1]
        step_size = min(size, 8)

        def some(step, carry):
            for i in range(step_size):
                at = first + step * step_size + i
                total = block_sum(sums, pointers, piece * per_piece + at)
                if more is not None:
                    total = total + more[at].astype(jnp.float32)
                partial[piece, at] = total.astype(partial.dtype)
            return carry

        lax.fori_loop(0, size // step_size, some, 0)

    def along(first, last):
        for far in range(first, last, 1 if last > first else -1):
            for sign in (1, -1):
                other = row + sign * far
                yield far, sign, (other >= 0) & (other < rows), other

    end = rows - 1
    chunks = sum_one_sem.shape[1]
    share = partial_one.shape[1] // sum(SPLIT)
    starts = [sum(SPLIT[:h]) * share for h in range(chunks)]
    sizes = [part * share for part in SPLIT]
    parts = [pl.ds(start, size) for start, size in zip(starts, sizes)]

    def sum_copy(h, other):
        return copy_to(
            partial_one.at[other, parts[h]],
            arrived_one.at[row, parts[h]],
            sum_one_sem.at[0, h, other],
            sum_one_sem.at[1, h, row],
            {"row": other},
        )

    def sum_wait(h, other):
        return copy_to(
            partial_one.at[other, parts[h]],
            arrived_one.at[other, parts[h]],
            sum_one_sem.at[0, h, other],
            sum_one_sem.at[1, h, other],
            {"row": other},
        )

    def pass_copy(h, side, other, through):
        return copy_to(
            partial_one.at[other, parts[h]],
            passing.at[side, parts[h]],
            pass_sem.at[0, side, h],
            pass_sem.at[1, side, h],
            {"row": through},
        )

    sides = [(0, 0, 1, end), (1, end, end - 1, 0)]
    for h in range(chunks):
        with jax.named_scope(f"partials#h={h}"):
            for side, source, through, to in sides:

                @pl.when(row == source)
                def _():
                    partials(sums_one, pointers_one, partial_one, to, starts[h], sizes[h])
                    pass_copy(h, side, to, through).start()

            for far, sign, valid, other in along(end - 1, 0):
                direct = valid
                if far == end - 1:
                    to = end if sign > 0 else 0
                    direct = valid & (other != to)

                @pl.when(direct)
                def _():
                    partials(sums_one, pointers_one, partial_one, other, starts[h], sizes[h])
                    sum_copy(h, other).start()

    def pass_on(h):
        for side, source, through, to in sides:

            @pl.when(row == through)
            def _():
                pass_copy(h, side, to, through).wait_recv()
                partials(sums_one, pointers_one, partial_one, to, starts[h], sizes[h], passing.at[side])
                sum_copy(h, to).start()

    def own_copy(h, piece, other, out_sem):
        return copy_to(
            group_one.at[piece, parts[h]],
            group_one.at[piece, parts[h]],
            out_sem,
            own_one_sem.at[1, h, piece],
            {"row": other},
        )

    def own_direct(far, other):
        if far == 1:
            return True
        return (other != 0) & (other != end)

    for h in range(chunks):
        with jax.named_scope(f"pass#h={h}"):
            pass_on(h)
        for far, sign, valid, other in along(1, rows):
            if far == end:
                continue

            @pl.when(valid)
            def _():
                with jax.named_scope(f"wait_sum#h={h}#far={far}"):
                    sum_wait(h, other).wait_recv()

        with jax.named_scope(f"own#h={h}"):
            base = row * partial_one.shape[1]

            def finish(i):
                at = starts[h] + i
                total = block_sum(sums_one, pointers_one, base + at) + injected_one[at]
                for other in range(rows):
                    comes = (row != other) & ((row - other) * (row - other) < end * end)
                    here = arrived_one[other, at].astype(jnp.float32)
                    total = total + jnp.where(comes, here, 0.0)
                value = total.astype(out_one.dtype)
                out_one[:, at * edge : (at + 1) * edge] = value
                group_one[row, at] = value

            for i in range(sizes[h]):
                finish(i)
            for far, sign, valid, other in along(end, 0):

                @pl.when(valid & own_direct(far, other))
                def _():
                    own_copy(h, row, other, own_one_sem.at[0, h, other]).start()

    def points_at_two(first, last):
        with jax.named_scope("points_two"):
            points_groups(
                first,
                last,
                points_two,
                lambda j: group_one[row, j],
                group_one.shape[1],
                min(group_one.shape[1], 32),
                injected_two,
            )

    groups_two = points_two.shape[0]
    for h in range(chunks):
        for far in range(1, rows):
            for sign in (1, -1):
                other = row + sign * far
                valid = (other >= 0) & (other < rows)
                with jax.named_scope(f"wait_own#h={h}#far={far}"):

                    @pl.when(valid)
                    def _():
                        own_copy(h, other, row, own_one_sem.at[0, h, other]).wait_recv()

                    for to, through in ((end, end - 1), (0, 1)):

                        @pl.when(valid & (row == through) & ((other - to) * (other - to) > 1) & (other != to))
                        def _():
                            own_copy(h, other, to, on_sem.at[h, other]).start()

            if h == 0:
                points_at_two(groups_two * (far - 1) // end, groups_two * far // end)

    def drain_one():
        for h in range(chunks):
            for side, source, through, to in sides:

                @pl.when(row == source)
                def _():
                    pass_copy(h, side, to, through).wait_send()

                @pl.when(row == through)
                def _():
                    sum_copy(h, to).wait_send()

            for far, sign, valid, other in along(end - 1, 0):
                direct = valid
                if far == end - 1:
                    to = end if sign > 0 else 0
                    direct = valid & (other != to)

                @pl.when(direct)
                def _():
                    sum_copy(h, other).wait_send()

            for far, sign, valid, other in along(end, 0):

                @pl.when(valid & own_direct(far, other))
                def _():
                    own_copy(h, row, other, own_one_sem.at[0, h, other]).wait_send()

                for to, through in ((end, end - 1), (0, 1)):

                    @pl.when(valid & (row == through) & ((other - to) * (other - to) > 1) & (other != to))
                    def _():
                        own_copy(h, other, to, on_sem.at[h, other]).wait_send()

    def exchange(sums, pointers, partial, arrived, injected, peers, axis, me, sems, group, own_sems, out):
        size = partial.shape[1]
        first, again = [], []
        with jax.named_scope("partials"):
            for k, peer in peers:
                partials(sums, pointers, partial, peer, 0, size)
                first.append(send(partial.at[peer], arrived.at[k - 1], sems, (k - 1,), {axis: peer}))
        own = [block_sum(sums, pointers, me * size + i) + injected[i] for i in range(size)]
        for (k, _), copy in zip(peers, first):
            with jax.named_scope(f"wait_sum#k={k}"):
                copy.wait_recv()
            for i in range(size):
                own[i] = own[i] + arrived[k - 1, i].astype(jnp.float32)
        for i in range(size):
            value = own[i].astype(out.dtype)
            out[:, i * edge : (i + 1) * edge] = value
            if group is not None:
                group[me, i] = value
        if group is not None:
            for k, peer in peers:
                again.append(send(group.at[me], group.at[me], own_sems, (k - 1,), {axis: peer}))
        return first, again

    def restrict(held, columns, group, sums):
        number = held.shape[0]
        batch = min(2 * BATCH, number)
        per_piece = group.shape[1]

        def some(step, total):
            first = step * batch

            def source_of(i):
                column = columns[first + i]
                return group[jnp.right_shift(column, shift_of(per_piece)), jnp.bitwise_and(column, per_piece - 1)]

            found = some_products(held, batch, lambda i: first + i, source_of)
            for i, product in enumerate(found):
                total = total + product
                sums[first + i + 1] = total
            return total

        sums[0] = jnp.zeros(sums.shape[1:], jnp.float32)
        lax.fori_loop(0, number // batch, some, jnp.zeros(sums.shape[1:], jnp.float32))

    with jax.named_scope("restrict_two"):
        restrict(held_two, columns_two, group_one, sums_two)
    sent_two, own_two = exchange(
        sums_two, pointers_two, partial_two, arrived_two, injected_two, far_peers, "col", col, sum_two_sem, group_two,
        own_two_sem, out_two,
    )
    with jax.named_scope("points_three"):
        points_groups(
            0,
            points_three.shape[0],
            points_three,
            lambda j: group_two[col, j],
            group_two.shape[1],
            group_two.shape[1],
            injected_three,
        )
    with jax.named_scope("wait_group_two"):
        for copy in own_two:
            copy.wait_recv()
    with jax.named_scope("restrict_three"):
        restrict(held_three, columns_three, group_two, sums_three)
    sent_three, _ = exchange(
        sums_three, pointers_three, partial_three, arrived_three, injected_three, row_peers, "row", row, sum_three_sem,
        None, None, out_three,
    )
    with jax.named_scope("drain"):
        for copy in asks + answers + sent_two + own_two + sent_three:
            copy.wait_send()
        drain_one()


def tail_kernel(*refs):
    half = len(refs) // 2
    for source, out in zip(refs[:half], refs[half:]):
        out[...] = source[...]


def on_device(
    fine_residual,
    tiles_one,
    pointers_one,
    columns_one,
    points_one,
    tiles_two,
    pointers_two,
    columns_two,
    points_two,
    tiles_three,
    pointers_three,
    columns_three,
    points_three,
):
    vectors = fine_residual.shape[0]
    edge = tiles_one.shape[1]
    rows, cols = lax.axis_size("row"), lax.axis_size("col")
    slots = tiles_one.shape[0]
    per_peer = slots // cols
    low, wide = fine_residual.dtype, jnp.float32
    piece_one = (pointers_one.shape[0] - 1) // rows
    piece_two = (pointers_two.shape[0] - 1) // cols
    piece_three = (pointers_three.shape[0] - 1) // rows
    chunks = len(SPLIT)

    def grouped(points):
        size = points.shape[0] // edge
        group = min(size, 2)
        return points.reshape(size // group, 1, group * edge)

    block = (vectors, edge)
    dma = pltpu.SemaphoreType.DMA
    inputs = [
        (fine_residual, pltpu.VMEM),
        (columns_one.reshape(1, slots), pltpu.VMEM),
        (pointers_one, pltpu.SMEM),
        (pointers_two, pltpu.SMEM),
        (pointers_three, pltpu.SMEM),
        (columns_two, pltpu.SMEM),
        (columns_three, pltpu.SMEM),
        (grouped(points_one), pltpu.VMEM),
        (grouped(points_two), pltpu.VMEM),
        (grouped(points_three), pltpu.VMEM),
        (tiles_one, pltpu.VMEM),
        (tiles_two, pltpu.VMEM),
        (tiles_three, pltpu.VMEM),
    ]
    scratch = [space(array.shape, array.dtype) for array, space in inputs]
    scratch += [
        pltpu.VMEM((1, slots), jnp.int32),
        pltpu.VMEM((1, slots), jnp.int32),
        pltpu.VMEM((1, slots), jnp.int32),
        pltpu.SMEM((1, slots), jnp.int32),
        pltpu.SMEM((1, slots), jnp.int32),
        pltpu.SMEM((cols, 1, slots), jnp.int32),
        pltpu.VMEM((fine_residual.shape[1] // edge,) + block, low),
        pltpu.VMEM((cols - 1, per_peer) + block, low),
        pltpu.VMEM((cols, per_peer) + block, low),
        pltpu.VMEM((slots,) + block, wide),
        pltpu.VMEM((slots + 1,) + block, wide),
        pltpu.VMEM((tiles_two.shape[0] + 1,) + block, wide),
        pltpu.VMEM((tiles_three.shape[0] + 1,) + block, wide),
        pltpu.VMEM((rows, piece_one) + block, low),
        pltpu.VMEM((cols, piece_two) + block, low),
        pltpu.VMEM((rows, piece_three) + block, low),
        pltpu.VMEM((rows, piece_one) + block, low),
        pltpu.VMEM((2, piece_one) + block, low),
        pltpu.VMEM((cols - 1, piece_two) + block, low),
        pltpu.VMEM((rows - 1, piece_three) + block, low),
        pltpu.VMEM((piece_one,) + block, wide),
        pltpu.VMEM((piece_two,) + block, wide),
        pltpu.VMEM((piece_three,) + block, wide),
        pltpu.VMEM((rows, piece_one) + block, low),
        pltpu.VMEM((cols, piece_two) + block, low),
        dma((len(inputs),)),
        dma((3,)),
        dma((2, cols - 1)),
        dma((2, cols - 1)),
        dma((2, chunks, rows)),
        dma((2, 2, chunks)),
        dma((2, chunks, rows)),
        dma((chunks, rows)),
        dma((2, cols - 1)),
        dma((2, cols - 1)),
        dma((2, rows - 1)),
    ]
    shapes = [jax.ShapeDtypeStruct((vectors, piece * edge), low) for piece in (piece_one, piece_two, piece_three)]
    vmem = [pl.BlockSpec(memory_space=pltpu.VMEM)] * 3
    found = pl.pallas_call(
        functools.partial(kernel, (rows, cols)),
        in_specs=[pl.BlockSpec(memory_space=pl.ANY)] * len(inputs),
        out_specs=vmem,
        out_shape=shapes,
        scratch_shapes=scratch,
        compiler_params=pltpu.CompilerParams(
            collective_id=0, has_side_effects=True
        ),
        name="restrict_all",
    )(*[array for array, _ in inputs])
    return pl.pallas_call(
        tail_kernel,
        in_specs=vmem,
        out_specs=vmem,
        out_shape=shapes,
        name="results",
    )(*found)


def solution(mesh):
    placed = (
        P(None, ("row", "col")),
        P(("row", "col"), None, None),
        P(("row", "col")),
        P(("row", "col")),
        P(("col", "row")),
        P(("row", "col"), None, None),
        P(("row", "col")),
        P(("row", "col")),
        P(("row", "col")),
        P(("row", "col"), None, None),
        P(("row", "col")),
        P(("row", "col")),
        P(("col", "row")),
    )
    return jax.shard_map(
        on_device,
        mesh=mesh,
        in_specs=placed,
        out_specs=(P(None, ("col", "row")), P(None, ("row", "col")), P(None, ("col", "row"))),
        check_vma=False,
    )
```

```python
import functools

import jax
import jax.numpy as jnp
from jax import lax
from jax.experimental import pallas as pl
from jax.experimental.pallas import tpu as pltpu
from jax.sharding import PartitionSpec as P

SPLIT = (1, 1, 1, 1)
BATCH = 16
LEAD = 0
STRAIGHT = 1


def mirrored(index, mask, count):
    flipped = index
    bit = 1
    while bit < count:
        if mask & bit:
            flipped = flipped + bit * (1 - 2 * lax.rem(index // bit, 2))
        bit *= 2
    return flipped


def mirror_order(count):
    return sorted(range(1, count), key=lambda mask: (bin(mask).count("1"), mask))


def far_order(count):
    return sorted(range(1, count), key=lambda mask: (-bin(mask >> 1).count("1"), mask & 1, mask))


def shift_of(size):
    assert size & (size - 1) == 0
    return size.bit_length() - 1


def down(row):
    edge = 128
    parts = []
    for first in range(0, row.shape[1], edge):
        spread = jnp.broadcast_to(row[:, first : first + edge], (edge, edge))
        parts.append(jnp.transpose(spread, (1, 0)))
    return parts


def plan(columns_ref, live, peers, blocks_peer, requests_ref, slots_ref, targets_ref):
    slots = columns_ref.shape[1]
    edge = 128
    per_peer = slots // peers
    columns = columns_ref[...]
    places = lax.broadcasted_iota(jnp.int32, (1, slots), 1)
    owner = jnp.right_shift(columns, shift_of(blocks_peer))
    within = jnp.bitwise_and(columns, blocks_peer - 1)
    owner = jnp.where(places < live, owner, peers + places)
    rank = jnp.zeros((1, slots), jnp.int32)
    owners_down = down(owner)
    for part, other in enumerate(owners_down):
        lines = lax.broadcasted_iota(jnp.int32, (edge, edge), 0) + part * edge
        ranks = []
        for first in range(0, slots, edge):
            lanes = lax.broadcasted_iota(jnp.int32, (edge, edge), 1) + first
            here = jnp.broadcast_to(owner[:, first : first + edge], (edge, edge))
            same = jnp.where((other == here) & (lines < lanes), 1, 0)
            ranks.append(jnp.sum(same, axis=0, keepdims=True))
        rank = rank + jnp.concatenate(ranks, axis=1)
    target = jnp.where(places < live, owner * per_peer + rank, slots)
    targets_ref[...] = jnp.where(places < live, target, 0)
    targets_down = down(target)
    within_down = down(within)
    for first in range(0, slots, edge):
        lanes = lax.broadcasted_iota(jnp.int32, (edge, edge), 1) + first
        request = jnp.zeros((1, edge), jnp.int32)
        slot = jnp.zeros((1, edge), jnp.int32)
        for part in range(slots // edge):
            lines = lax.broadcasted_iota(jnp.int32, (edge, edge), 0) + part * edge
            hit = targets_down[part] == lanes
            request = request + jnp.sum(jnp.where(hit, within_down[part], 0), axis=0, keepdims=True)
            slot = slot + jnp.sum(jnp.where(hit, lines, 0), axis=0, keepdims=True)
        requests_ref[:, first : first + edge] = request
        slots_ref[:, first : first + edge] = slot


def pair_products(tiles, sources):
    none = jnp.zeros_like(sources[0])
    left = jnp.concatenate([sources[0], none], axis=1)
    right = jnp.concatenate([none, sources[1]], axis=1)
    both = lax.dot_general(
        jnp.concatenate([left, right], axis=0),
        jnp.concatenate(tiles, axis=1),
        (((1,), (1,)), ((), ())),
        preferred_element_type=jnp.float32,
    )
    vectors = sources[0].shape[0]
    return both[:vectors], both[vectors:]


def some_products(tiles_ref, number, tile_of, source_of):
    products = []
    for i in range(0, number, 2):
        products += pair_products(
            [tiles_ref[tile_of(i)], tiles_ref[tile_of(i + 1)]], [source_of(i), source_of(i + 1)]
        )
    return products


def points_groups(first, last, points_ref, block_of, blocks, span, out_ref):
    edge = out_ref.shape[2]
    vectors = out_ref.shape[1]
    wide = points_ref.shape[2]
    group = wide // edge

    def one_group(number, carry):
        points = points_ref[number]
        owners = jnp.broadcast_to(jnp.right_shift(points, shift_of(edge)), (vectors, wide))
        lanes = jnp.broadcast_to(jnp.bitwise_and(points, edge - 1), (edge, wide))
        spots = lax.broadcasted_iota(jnp.int32, (edge, wide), 0)
        pick = (lanes == spots).astype(jnp.float32).astype(jnp.bfloat16)
        found = jnp.zeros((vectors, wide), jnp.float32)
        for part in range(blocks // span):
            rows = jnp.concatenate([block_of(part * span + k) for k in range(span)], axis=0)
            moved = jnp.dot(rows, pick, preferred_element_type=jnp.float32)
            for k in range(span):
                here = moved[k * vectors : (k + 1) * vectors]
                found = jnp.where(owners == part * span + k, here, found)
        for i in range(group):
            out_ref[number * group + i] = found[:, i * edge : (i + 1) * edge]
        return carry

    lax.fori_loop(first, last, one_group, 0)


def kernel(axes, *refs):
    rows, cols = axes
    (fine_h, columns_h, pointers_one_h, pointers_two_h, pointers_three_h, columns_two_h, columns_three_h) = refs[:7]
    (points_one_h, points_two_h, points_three_h, tiles_one, tiles_two, tiles_three) = refs[7:13]
    out_one, out_two, out_three = refs[13:16]
    (fine_ref, columns_ref, pointers_one, pointers_two, pointers_three, columns_two, columns_three) = refs[16:23]
    (points_one, points_two, points_three, held_one, held_two, held_three) = refs[23:29]
    (requests_v, slots_v, targets_v, slots_s, targets_s, asked_s) = refs[29:35]
    (fine_blocks, replies_out, replies, products_one, sums_one, sums_two, sums_three) = refs[35:42]
    (partial_one, partial_two, partial_three, arrived_one, passing, arrived_two, arrived_three) = refs[42:49]
    (injected_one, injected_two, injected_three, group_one, group_two) = refs[49:54]
    (load_sem, local_sem, request_sem, reply_sem, sum_one_sem, pass_sem, own_one_sem, on_sem) = refs[54:62]
    (sum_two_sem, own_two_sem, sum_three_sem) = refs[62:]

    row, col = lax.axis_index("row"), lax.axis_index("col")
    edge = held_one.shape[2]
    slots = columns_ref.shape[1]
    per_peer = slots // cols
    blocks_peer = fine_ref.shape[1] // edge
    row_peers = [(k, lax.rem(row + k, rows)) for k in range(1, rows)]
    col_peers = [(m, mirrored(col, m, cols)) for m in mirror_order(cols)]
    far_peers = [(m, mirrored(col, m, cols)) for m in far_order(cols)]
    mesh_id = pl.DeviceIdType.MESH

    barrier = pltpu.get_barrier_semaphore()
    for _, peer in row_peers:
        pl.semaphore_signal(barrier, inc=1, device_id={"row": peer}, device_id_type=mesh_id)
    for _, peer in col_peers:
        pl.semaphore_signal(barrier, inc=1, device_id={"col": peer}, device_id_type=mesh_id)
    pairs = [
        (columns_h, columns_ref),
        (pointers_one_h, pointers_one),
        (fine_h, fine_ref),
        (points_one_h, points_one),
        (tiles_one, held_one),
        (pointers_two_h, pointers_two),
        (pointers_three_h, pointers_three),
        (columns_two_h, columns_two),
        (columns_three_h, columns_three),
        (points_two_h, points_two),
        (points_three_h, points_three),
        (tiles_two, held_two),
        (tiles_three, held_three),
    ]
    loads = [
        pltpu.make_async_copy(source, held, load_sem.at[i]) for i, (source, held) in enumerate(pairs)
    ]
    for load in loads:
        load.start()

    with jax.named_scope("wait_plan"):
        loads[0].wait()
        loads[1].wait()
    with jax.named_scope("plan"):
        plan(
            columns_ref,
            pointers_one[pointers_one.shape[0] - 1],
            cols,
            blocks_peer,
            requests_v,
            slots_v,
            targets_v,
        )
    plans = [
        pltpu.make_async_copy(requests_v, asked_s.at[0], local_sem.at[0]),
        pltpu.make_async_copy(slots_v, slots_s, local_sem.at[1]),
        pltpu.make_async_copy(targets_v, targets_s, local_sem.at[2]),
    ]
    with jax.named_scope("barrier"):
        pl.semaphore_wait(barrier, rows + cols - 2)

    def copy_to(source, target, out_sem, in_sem, device):
        return pltpu.make_async_remote_copy(
            src_ref=source,
            dst_ref=target,
            send_sem=out_sem,
            recv_sem=in_sem,
            device_id=device,
            device_id_type=mesh_id,
        )

    def send(source, target, sems, at, device):
        copy = copy_to(source, target, sems.at[(0,) + at], sems.at[(1,) + at], device)
        copy.start()
        return copy

    asks = [send(requests_v, asked_s.at[m], request_sem, (m - 1,), {"col": peer}) for m, peer in col_peers]
    for copy in plans:
        copy.start()

    def take(m, out_ref, place):
        base = col * per_peer

        def some(step, carry):
            for i in range(8):
                at = step * 8 + i
                out_ref[place, at] = fine_blocks[asked_s[m, 0, base + at]]
            return carry

        lax.fori_loop(0, per_peer // 8, some, 0)

    def products_of(m, owner):
        base = owner * per_peer
        batch = min(BATCH, per_peer)

        def some(step, carry):
            first = step * batch
            found = some_products(
                held_one,
                batch,
                lambda i: slots_s[0, base + first + i],
                lambda i: replies[m, first + i],
            )
            for i, product in enumerate(found):
                products_one[base + first + i] = product
            return carry

        lax.fori_loop(0, per_peer // batch, some, 0)

    groups = points_one.shape[0]
    span_one = min(blocks_peer, 32)
    marks = [groups * part // 16 for part in (0, 5, 9, 13, 16)]

    def points_at_one(part):
        with jax.named_scope("points_one"):
            points_groups(
                marks[part],
                marks[part + 1],
                points_one,
                lambda j: fine_blocks[j],
                blocks_peer,
                span_one,
                injected_one,
            )

    with jax.named_scope("wait_fine"):
        loads[2].wait()
        loads[3].wait()
    with jax.named_scope("blocks"):
        for j in range(blocks_peer):
            fine_blocks[j] = fine_ref[:, j * edge : (j + 1) * edge]
    points_at_one(0)
    with jax.named_scope("wait_ask"):
        for copy in asks:
            copy.wait_recv()
        for copy in plans:
            copy.wait()
        take(0, replies, 0)
    answers = []
    with jax.named_scope("answer"):
        for m, peer in col_peers:
            take(m, replies_out, m - 1)
            answers.append(send(replies_out.at[m - 1], replies.at[m], reply_sem, (m - 1,), {"col": peer}))
    with jax.named_scope("wait_tiles"):
        loads[4].wait()
    products_of(0, col)
    points_at_one(1)
    coming = list(zip(col_peers, answers))
    for number, ((m, peer), copy) in enumerate(coming):
        with jax.named_scope(f"wait_reply#m={m}"):
            copy.wait_recv()
        with jax.named_scope(f"products#m={m}"):
            products_of(m, peer)
        if number + 2 < len(marks) - 1:
            points_at_one(number + 2)
    for load in loads[5:]:
        load.wait()

    def run_one(step, total):
        for i in range(8):
            at = step * 8 + i
            total = total + products_one[targets_s[0, at]]
            sums_one[at + 1] = total
        return total

    with jax.named_scope("run_one"):
        sums_one[0] = jnp.zeros(sums_one.shape[1:], jnp.float32)
        lax.fori_loop(0, slots // 8, run_one, jnp.zeros(sums_one.shape[1:], jnp.float32))

    def block_sum(sums, pointers, block):
        return sums[pointers[block + 1]] - sums[pointers[block]]

    def partials(sums, pointers, partial, piece, first, size, more=None):
        per_piece = partial.shape[1]
        step_size = min(size, 8)

        def some(step, carry):
            for i in range(step_size):
                at = first + step * step_size + i
                total = block_sum(sums, pointers, piece * per_piece + at)
                if more is not None:
                    total = total + more[at].astype(jnp.float32)
                partial[piece, at] = total.astype(partial.dtype)
            return carry

        lax.fori_loop(0, size // step_size, some, 0)

    def along(first, last):
        for far in range(first, last, 1 if last > first else -1):
            for sign in (1, -1):
                other = row + sign * far
                yield far, sign, (other >= 0) & (other < rows), other

    end = rows - 1
    chunks = sum_one_sem.shape[1]
    share = partial_one.shape[1] // sum(SPLIT)
    starts = [sum(SPLIT[:h]) * share for h in range(chunks)]
    sizes = [part * share for part in SPLIT]
    parts = [pl.ds(start, size) for start, size in zip(starts, sizes)]

    def sum_copy(h, other):
        return copy_to(
            partial_one.at[other, parts[h]],
            arrived_one.at[row, parts[h]],
            sum_one_sem.at[0, h, other],
            sum_one_sem.at[1, h, row],
            {"row": other},
        )

    def sum_wait(h, other):
        return copy_to(
            partial_one.at[other, parts[h]],
            arrived_one.at[other, parts[h]],
            sum_one_sem.at[0, h, other],
            sum_one_sem.at[1, h, other],
            {"row": other},
        )

    def pass_copy(h, side, other, through):
        return copy_to(
            partial_one.at[other, parts[h]],
            passing.at[side, parts[h]],
            pass_sem.at[0, side, h],
            pass_sem.at[1, side, h],
            {"row": through},
        )

    sides = [(0, 0, 1, end), (1, end, end - 1, 0)]
    def send_ends(h):
        for side, source, through, to in sides:

            @pl.when(row == source)
            def _():
                partials(sums_one, pointers_one, partial_one, to, starts[h], sizes[h])
                pass_copy(h, side, to, through).start()

    def send_sums(h):
        for far, sign, valid, other in along(end - 1, 0):
            direct = valid
            if far == end - 1:
                to = end if sign > 0 else 0
                direct = valid & (other != to)

            @pl.when(direct)
            def _():
                partials(sums_one, pointers_one, partial_one, other, starts[h], sizes[h])
                sum_copy(h, other).start()

    for h in range(chunks + LEAD):
        with jax.named_scope(f"partials#h={h}"):
            if h < chunks:
                send_ends(h)
            if h >= LEAD:
                send_sums(h - LEAD)

    def pass_on(h):
        for side, source, through, to in sides:

            @pl.when(row == through)
            def _():
                pass_copy(h, side, to, through).wait_recv()
                partials(sums_one, pointers_one, partial_one, to, starts[h], sizes[h], passing.at[side])
                sum_copy(h, to).start()

    def own_copy(h, piece, other, out_sem):
        return copy_to(
            group_one.at[piece, parts[h]],
            group_one.at[piece, parts[h]],
            out_sem,
            own_one_sem.at[1, h, piece],
            {"row": other},
        )

    def straight(h):
        return h >= chunks - STRAIGHT

    def own_direct(h, far, other):
        if far == 1 or (far == end and straight(h)):
            return True
        return (other != 0) & (other != end)

    def sum_up(h):
        with jax.named_scope(f"pass#h={h}"):
            pass_on(h)
        for far, sign, valid, other in along(1, rows):
            if far == end:
                continue

            @pl.when(valid)
            def _():
                with jax.named_scope(f"wait_sum#h={h}#far={far}"):
                    sum_wait(h, other).wait_recv()

        with jax.named_scope(f"own#h={h}"):
            base = row * partial_one.shape[1]

            def finish(i):
                at = starts[h] + i
                total = block_sum(sums_one, pointers_one, base + at) + injected_one[at]
                for other in range(rows):
                    comes = (row != other) & ((row - other) * (row - other) < end * end)
                    here = arrived_one[other, at].astype(jnp.float32)
                    total = total + jnp.where(comes, here, 0.0)
                value = total.astype(out_one.dtype)
                out_one[:, at * edge : (at + 1) * edge] = value
                group_one[row, at] = value

            for i in range(sizes[h]):
                finish(i)
            for far, sign, valid, other in along(end, 0):

                @pl.when(valid & own_direct(h, far, other))
                def _():
                    own_copy(h, row, other, own_one_sem.at[0, h, other]).start()

    def points_at_two(first, last):
        with jax.named_scope("points_two"):
            points_groups(
                first,
                last,
                points_two,
                lambda j: group_one[row, j],
                group_one.shape[1],
                min(group_one.shape[1], 32),
                injected_two,
            )

    def onwards(h, valid, other):
        for to, through in ((end, end - 1), (0, 1)):
            gap = (other - to) * (other - to)
            onward = valid & (row == through) & (gap > 1)
            if straight(h):
                onward = onward & (gap < end * end)
            yield to, onward

    def early(h, valid, other):
        passed = False
        for _, onward in onwards(h, valid, other):
            passed = passed | onward
        return passed & (other != 0) & (other != end)

    def receive(h, other, wanted):
        @pl.when(wanted)
        def _():
            own_copy(h, other, row, own_one_sem.at[0, h, other]).wait_recv()

        for to, onward in onwards(h, wanted, other):

            @pl.when(onward)
            def _():
                own_copy(h, other, to, on_sem.at[h, other]).start()

    def receive_early(h):
        for far, sign, valid, other in along(1, rows):
            receive(h, other, early(h, valid, other))

    for h in range(chunks):
        sum_up(h)
        if h > 0:
            receive_early(h - 1)
    receive_early(chunks - 1)

    groups_two = points_two.shape[0]
    for h in range(chunks):
        for far in range(1, rows):
            for sign in (1, -1):
                other = row + sign * far
                valid = (other >= 0) & (other < rows)
                with jax.named_scope(f"wait_own#h={h}#far={far}"):
                    receive(h, other, valid & jnp.logical_not(early(h, valid, other)))
            if h == 0:
                points_at_two(groups_two * (far - 1) // end, groups_two * far // end)

    def drain_one():
        for h in range(chunks):
            for side, source, through, to in sides:

                @pl.when(row == source)
                def _():
                    pass_copy(h, side, to, through).wait_send()

                @pl.when(row == through)
                def _():
                    sum_copy(h, to).wait_send()

            for far, sign, valid, other in along(end - 1, 0):
                direct = valid
                if far == end - 1:
                    to = end if sign > 0 else 0
                    direct = valid & (other != to)

                @pl.when(direct)
                def _():
                    sum_copy(h, other).wait_send()

            for far, sign, valid, other in along(end, 0):

                @pl.when(valid & own_direct(h, far, other))
                def _():
                    own_copy(h, row, other, own_one_sem.at[0, h, other]).wait_send()

                for to, onward in onwards(h, valid, other):

                    @pl.when(onward)
                    def _():
                        own_copy(h, other, to, on_sem.at[h, other]).wait_send()

    def exchange(sums, pointers, partial, arrived, injected, peers, axis, me, sems, group, own_sems, out):
        size = partial.shape[1]
        first, again = [], []
        with jax.named_scope("partials"):
            for k, peer in peers:
                partials(sums, pointers, partial, peer, 0, size)
                first.append(send(partial.at[peer], arrived.at[k - 1], sems, (k - 1,), {axis: peer}))
        own = [block_sum(sums, pointers, me * size + i) + injected[i] for i in range(size)]
        for (k, _), copy in zip(peers, first):
            with jax.named_scope(f"wait_sum#k={k}"):
                copy.wait_recv()
            for i in range(size):
                own[i] = own[i] + arrived[k - 1, i].astype(jnp.float32)
        for i in range(size):
            value = own[i].astype(out.dtype)
            out[:, i * edge : (i + 1) * edge] = value
            if group is not None:
                group[me, i] = value
        if group is not None:
            for k, peer in peers:
                again.append(send(group.at[me], group.at[me], own_sems, (k - 1,), {axis: peer}))
        return first, again

    def restrict(held, columns, group, sums):
        number = held.shape[0]
        batch = min(2 * BATCH, number)
        per_piece = group.shape[1]

        def some(step, total):
            first = step * batch

            def source_of(i):
                column = columns[first + i]
                return group[jnp.right_shift(column, shift_of(per_piece)), jnp.bitwise_and(column, per_piece - 1)]

            found = some_products(held, batch, lambda i: first + i, source_of)
            for i, product in enumerate(found):
                total = total + product
                sums[first + i + 1] = total
            return total

        sums[0] = jnp.zeros(sums.shape[1:], jnp.float32)
        lax.fori_loop(0, number // batch, some, jnp.zeros(sums.shape[1:], jnp.float32))

    with jax.named_scope("restrict_two"):
        restrict(held_two, columns_two, group_one, sums_two)
    sent_two, own_two = exchange(
        sums_two, pointers_two, partial_two, arrived_two, injected_two, far_peers, "col", col, sum_two_sem, group_two,
        own_two_sem, out_two,
    )
    with jax.named_scope("points_three"):
        points_groups(
            0,
            points_three.shape[0],
            points_three,
            lambda j: group_two[col, j],
            group_two.shape[1],
            group_two.shape[1],
            injected_three,
        )
    with jax.named_scope("wait_group_two"):
        for copy in own_two:
            copy.wait_recv()
    with jax.named_scope("restrict_three"):
        restrict(held_three, columns_three, group_two, sums_three)
    sent_three, _ = exchange(
        sums_three, pointers_three, partial_three, arrived_three, injected_three, row_peers, "row", row, sum_three_sem,
        None, None, out_three,
    )
    with jax.named_scope("drain"):
        for copy in asks + answers + sent_two + own_two + sent_three:
            copy.wait_send()
        drain_one()


def tail_kernel(*refs):
    half = len(refs) // 2
    for source, out in zip(refs[:half], refs[half:]):
        out[...] = source[...]


def on_device(
    fine_residual,
    tiles_one,
    pointers_one,
    columns_one,
    points_one,
    tiles_two,
    pointers_two,
    columns_two,
    points_two,
    tiles_three,
    pointers_three,
    columns_three,
    points_three,
):
    vectors = fine_residual.shape[0]
    edge = tiles_one.shape[1]
    rows, cols = lax.axis_size("row"), lax.axis_size("col")
    slots = tiles_one.shape[0]
    per_peer = slots // cols
    low, wide = fine_residual.dtype, jnp.float32
    piece_one = (pointers_one.shape[0] - 1) // rows
    piece_two = (pointers_two.shape[0] - 1) // cols
    piece_three = (pointers_three.shape[0] - 1) // rows
    chunks = len(SPLIT)

    def grouped(points):
        size = points.shape[0] // edge
        group = min(size, 2)
        return points.reshape(size // group, 1, group * edge)

    block = (vectors, edge)
    dma = pltpu.SemaphoreType.DMA
    inputs = [
        (fine_residual, pltpu.VMEM),
        (columns_one.reshape(1, slots), pltpu.VMEM),
        (pointers_one, pltpu.SMEM),
        (pointers_two, pltpu.SMEM),
        (pointers_three, pltpu.SMEM),
        (columns_two, pltpu.SMEM),
        (columns_three, pltpu.SMEM),
        (grouped(points_one), pltpu.VMEM),
        (grouped(points_two), pltpu.VMEM),
        (grouped(points_three), pltpu.VMEM),
        (tiles_one, pltpu.VMEM),
        (tiles_two, pltpu.VMEM),
        (tiles_three, pltpu.VMEM),
    ]
    scratch = [space(array.shape, array.dtype) for array, space in inputs]
    scratch += [
        pltpu.VMEM((1, slots), jnp.int32),
        pltpu.VMEM((1, slots), jnp.int32),
        pltpu.VMEM((1, slots), jnp.int32),
        pltpu.SMEM((1, slots), jnp.int32),
        pltpu.SMEM((1, slots), jnp.int32),
        pltpu.SMEM((cols, 1, slots), jnp.int32),
        pltpu.VMEM((fine_residual.shape[1] // edge,) + block, low),
        pltpu.VMEM((cols - 1, per_peer) + block, low),
        pltpu.VMEM((cols, per_peer) + block, low),
        pltpu.VMEM((slots,) + block, wide),
        pltpu.VMEM((slots + 1,) + block, wide),
        pltpu.VMEM((tiles_two.shape[0] + 1,) + block, wide),
        pltpu.VMEM((tiles_three.shape[0] + 1,) + block, wide),
        pltpu.VMEM((rows, piece_one) + block, low),
        pltpu.VMEM((cols, piece_two) + block, low),
        pltpu.VMEM((rows, piece_three) + block, low),
        pltpu.VMEM((rows, piece_one) + block, low),
        pltpu.VMEM((2, piece_one) + block, low),
        pltpu.VMEM((cols - 1, piece_two) + block, low),
        pltpu.VMEM((rows - 1, piece_three) + block, low),
        pltpu.VMEM((piece_one,) + block, wide),
        pltpu.VMEM((piece_two,) + block, wide),
        pltpu.VMEM((piece_three,) + block, wide),
        pltpu.VMEM((rows, piece_one) + block, low),
        pltpu.VMEM((cols, piece_two) + block, low),
        dma((len(inputs),)),
        dma((3,)),
        dma((2, cols - 1)),
        dma((2, cols - 1)),
        dma((2, chunks, rows)),
        dma((2, 2, chunks)),
        dma((2, chunks, rows)),
        dma((chunks, rows)),
        dma((2, cols - 1)),
        dma((2, cols - 1)),
        dma((2, rows - 1)),
    ]
    shapes = [jax.ShapeDtypeStruct((vectors, piece * edge), low) for piece in (piece_one, piece_two, piece_three)]
    vmem = [pl.BlockSpec(memory_space=pltpu.VMEM)] * 3
    found = pl.pallas_call(
        functools.partial(kernel, (rows, cols)),
        in_specs=[pl.BlockSpec(memory_space=pl.ANY)] * len(inputs),
        out_specs=vmem,
        out_shape=shapes,
        scratch_shapes=scratch,
        compiler_params=pltpu.CompilerParams(
            collective_id=0, has_side_effects=True
        ),
        name="restrict_all",
    )(*[array for array, _ in inputs])
    return pl.pallas_call(
        tail_kernel,
        in_specs=vmem,
        out_specs=vmem,
        out_shape=shapes,
        name="results",
    )(*found)


def solution(mesh):
    placed = (
        P(None, ("row", "col")),
        P(("row", "col"), None, None),
        P(("row", "col")),
        P(("row", "col")),
        P(("col", "row")),
        P(("row", "col"), None, None),
        P(("row", "col")),
        P(("row", "col")),
        P(("row", "col")),
        P(("row", "col"), None, None),
        P(("row", "col")),
        P(("row", "col")),
        P(("col", "row")),
    )
    return jax.shard_map(
        on_device,
        mesh=mesh,
        in_specs=placed,
        out_specs=(P(None, ("col", "row")), P(None, ("row", "col")), P(None, ("col", "row"))),
        check_vma=False,
    )
```

```python
import functools

import jax
import jax.numpy as jnp
from jax import lax
from jax.experimental import pallas as pl
from jax.experimental.pallas import tpu as pltpu
from jax.sharding import PartitionSpec as P

SPLIT = (1, 1, 1, 1)
BATCH = 16
LEAD = 0
STRAIGHT = 1


def mirrored(index, mask, count):
    flipped = index
    bit = 1
    while bit < count:
        if mask & bit:
            flipped = flipped + bit * (1 - 2 * lax.rem(index // bit, 2))
        bit *= 2
    return flipped


def mirror_order(count):
    return sorted(range(1, count), key=lambda mask: (bin(mask).count("1"), mask))


def far_order(count):
    return sorted(range(1, count), key=lambda mask: (-bin(mask >> 1).count("1"), mask & 1, mask))


def shift_of(size):
    assert size & (size - 1) == 0
    return size.bit_length() - 1


def down(row):
    edge = 128
    parts = []
    for first in range(0, row.shape[1], edge):
        spread = jnp.broadcast_to(row[:, first : first + edge], (edge, edge))
        parts.append(jnp.transpose(spread, (1, 0)))
    return parts


def plan(columns_ref, live, peers, blocks_peer, requests_ref, slots_ref, targets_ref):
    slots = columns_ref.shape[1]
    edge = 128
    per_peer = slots // peers
    columns = columns_ref[...]
    places = lax.broadcasted_iota(jnp.int32, (1, slots), 1)
    owner = jnp.right_shift(columns, shift_of(blocks_peer))
    within = jnp.bitwise_and(columns, blocks_peer - 1)
    owner = jnp.where(places < live, owner, peers + places)
    rank = jnp.zeros((1, slots), jnp.int32)
    owners_down = down(owner)
    for part, other in enumerate(owners_down):
        lines = lax.broadcasted_iota(jnp.int32, (edge, edge), 0) + part * edge
        ranks = []
        for first in range(0, slots, edge):
            lanes = lax.broadcasted_iota(jnp.int32, (edge, edge), 1) + first
            here = jnp.broadcast_to(owner[:, first : first + edge], (edge, edge))
            same = jnp.where((other == here) & (lines < lanes), 1, 0)
            ranks.append(jnp.sum(same, axis=0, keepdims=True))
        rank = rank + jnp.concatenate(ranks, axis=1)
    target = jnp.where(places < live, owner * per_peer + rank, slots)
    targets_ref[...] = jnp.where(places < live, target, 0)
    targets_down = down(target)
    within_down = down(within)
    for first in range(0, slots, edge):
        lanes = lax.broadcasted_iota(jnp.int32, (edge, edge), 1) + first
        request = jnp.zeros((1, edge), jnp.int32)
        slot = jnp.zeros((1, edge), jnp.int32)
        for part in range(slots // edge):
            lines = lax.broadcasted_iota(jnp.int32, (edge, edge), 0) + part * edge
            hit = targets_down[part] == lanes
            request = request + jnp.sum(jnp.where(hit, within_down[part], 0), axis=0, keepdims=True)
            slot = slot + jnp.sum(jnp.where(hit, lines, 0), axis=0, keepdims=True)
        requests_ref[:, first : first + edge] = request
        slots_ref[:, first : first + edge] = slot


def pair_products(tiles, sources):
    none = jnp.zeros_like(sources[0])
    left = jnp.concatenate([sources[0], none], axis=1)
    right = jnp.concatenate([none, sources[1]], axis=1)
    both = lax.dot_general(
        jnp.concatenate([left, right], axis=0),
        jnp.concatenate(tiles, axis=1),
        (((1,), (1,)), ((), ())),
        preferred_element_type=jnp.float32,
    )
    vectors = sources[0].shape[0]
    return both[:vectors], both[vectors:]


def some_products(tiles_ref, number, tile_of, source_of):
    products = []
    for i in range(0, number, 2):
        products += pair_products(
            [tiles_ref[tile_of(i)], tiles_ref[tile_of(i + 1)]], [source_of(i), source_of(i + 1)]
        )
    return products


def points_groups(first, last, points_ref, block_of, blocks, span, out_ref):
    edge = out_ref.shape[2]
    vectors = out_ref.shape[1]
    wide = points_ref.shape[2]
    group = wide // edge

    def one_group(number, carry):
        points = points_ref[number]
        owners = jnp.broadcast_to(jnp.right_shift(points, shift_of(edge)), (vectors, wide))
        lanes = jnp.broadcast_to(jnp.bitwise_and(points, edge - 1), (edge, wide))
        spots = lax.broadcasted_iota(jnp.int32, (edge, wide), 0)
        pick = (lanes == spots).astype(jnp.float32).astype(jnp.bfloat16)
        found = jnp.zeros((vectors, wide), jnp.float32)
        for part in range(blocks // span):
            rows = jnp.concatenate([block_of(part * span + k) for k in range(span)], axis=0)
            moved = jnp.dot(rows, pick, preferred_element_type=jnp.float32)
            for k in range(span):
                here = moved[k * vectors : (k + 1) * vectors]
                found = jnp.where(owners == part * span + k, here, found)
        for i in range(group):
            out_ref[number * group + i] = found[:, i * edge : (i + 1) * edge]
        return carry

    lax.fori_loop(first, last, one_group, 0)


def kernel(axes, *refs):
    rows, cols = axes
    (fine_h, columns_h, pointers_one_h, pointers_two_h, pointers_three_h, columns_two_h, columns_three_h) = refs[:7]
    (points_one_h, points_two_h, points_three_h, tiles_one, tiles_two, tiles_three) = refs[7:13]
    out_one, out_two, out_three = refs[13:16]
    (fine_ref, columns_ref, pointers_one, pointers_two, pointers_three, columns_two, columns_three) = refs[16:23]
    (points_one, points_two, points_three, held_one, held_two, held_three) = refs[23:29]
    (requests_v, slots_v, targets_v, slots_s, targets_s, asked_s) = refs[29:35]
    (fine_blocks, replies_out, replies, products_one, sums_one, sums_two, sums_three) = refs[35:42]
    (partial_one, partial_two, partial_three, arrived_one, passing, arrived_two, arrived_three) = refs[42:49]
    (injected_one, injected_two, injected_three, group_one, group_two) = refs[49:54]
    (load_sem, local_sem, request_sem, reply_sem, sum_one_sem, pass_sem, own_one_sem, on_sem) = refs[54:62]
    (sum_two_sem, own_two_sem, sum_three_sem) = refs[62:]

    row, col = lax.axis_index("row"), lax.axis_index("col")
    edge = held_one.shape[2]
    slots = columns_ref.shape[1]
    per_peer = slots // cols
    blocks_peer = fine_ref.shape[1] // edge
    row_peers = [(k, lax.rem(row + k, rows)) for k in range(1, rows)]
    col_peers = [(m, mirrored(col, m, cols)) for m in mirror_order(cols)]
    far_peers = [(m, mirrored(col, m, cols)) for m in far_order(cols)]
    mesh_id = pl.DeviceIdType.MESH

    barrier = pltpu.get_barrier_semaphore()
    for _, peer in row_peers:
        pl.semaphore_signal(barrier, inc=1, device_id={"row": peer}, device_id_type=mesh_id)
    for _, peer in col_peers:
        pl.semaphore_signal(barrier, inc=1, device_id={"col": peer}, device_id_type=mesh_id)
    pairs = [
        (columns_h, columns_ref),
        (pointers_one_h, pointers_one),
        (fine_h, fine_ref),
        (points_one_h, points_one),
        (tiles_one, held_one),
        (pointers_two_h, pointers_two),
        (pointers_three_h, pointers_three),
        (columns_two_h, columns_two),
        (columns_three_h, columns_three),
        (points_two_h, points_two),
        (points_three_h, points_three),
        (tiles_two, held_two),
        (tiles_three, held_three),
    ]
    loads = [
        pltpu.make_async_copy(source, held, load_sem.at[i]) for i, (source, held) in enumerate(pairs)
    ]
    for load in loads:
        load.start()

    with jax.named_scope("wait_plan"):
        loads[0].wait()
        loads[1].wait()
    with jax.named_scope("plan"):
        plan(
            columns_ref,
            pointers_one[pointers_one.shape[0] - 1],
            cols,
            blocks_peer,
            requests_v,
            slots_v,
            targets_v,
        )
    plans = [
        pltpu.make_async_copy(requests_v, asked_s.at[0], local_sem.at[0]),
        pltpu.make_async_copy(slots_v, slots_s, local_sem.at[1]),
        pltpu.make_async_copy(targets_v, targets_s, local_sem.at[2]),
    ]
    with jax.named_scope("barrier"):
        pl.semaphore_wait(barrier, rows + cols - 2)

    def copy_to(source, target, out_sem, in_sem, device):
        return pltpu.make_async_remote_copy(
            src_ref=source,
            dst_ref=target,
            send_sem=out_sem,
            recv_sem=in_sem,
            device_id=device,
            device_id_type=mesh_id,
        )

    def send(source, target, sems, at, device):
        copy = copy_to(source, target, sems.at[(0,) + at], sems.at[(1,) + at], device)
        copy.start()
        return copy

    asks = [send(requests_v, asked_s.at[m], request_sem, (m - 1,), {"col": peer}) for m, peer in col_peers]
    for copy in plans:
        copy.start()

    def take(m, out_ref, place):
        base = col * per_peer

        def some(step, carry):
            for i in range(8):
                at = step * 8 + i
                out_ref[place, at] = fine_blocks[asked_s[m, 0, base + at]]
            return carry

        lax.fori_loop(0, per_peer // 8, some, 0)

    def products_of(m, owner):
        base = owner * per_peer
        batch = min(BATCH, per_peer)

        def some(step, carry):
            first = step * batch
            found = some_products(
                held_one,
                batch,
                lambda i: slots_s[0, base + first + i],
                lambda i: replies[m, first + i],
            )
            for i, product in enumerate(found):
                products_one[base + first + i] = product
            return carry

        lax.fori_loop(0, per_peer // batch, some, 0)

    groups = points_one.shape[0]
    span_one = min(blocks_peer, 32)
    marks = [groups * part // 16 for part in (0, 5, 9, 13, 16)]

    def points_at_one(part):
        with jax.named_scope("points_one"):
            points_groups(
                marks[part],
                marks[part + 1],
                points_one,
                lambda j: fine_blocks[j],
                blocks_peer,
                span_one,
                injected_one,
            )

    with jax.named_scope("wait_fine"):
        loads[2].wait()
        loads[3].wait()
    with jax.named_scope("blocks"):
        for j in range(blocks_peer):
            fine_blocks[j] = fine_ref[:, j * edge : (j + 1) * edge]
    points_at_one(0)
    with jax.named_scope("wait_ask"):
        for copy in asks:
            copy.wait_recv()
    answers = []
    with jax.named_scope("answer"):
        for m, peer in col_peers:
            take(m, replies_out, m - 1)
            answers.append(send(replies_out.at[m - 1], replies.at[m], reply_sem, (m - 1,), {"col": peer}))
    for copy in plans:
        copy.wait()
    take(0, replies, 0)
    with jax.named_scope("wait_tiles"):
        loads[4].wait()
    products_of(0, col)
    points_at_one(1)
    coming = list(zip(col_peers, answers))
    for number, ((m, peer), copy) in enumerate(coming):
        with jax.named_scope(f"wait_reply#m={m}"):
            copy.wait_recv()
        with jax.named_scope(f"products#m={m}"):
            products_of(m, peer)
        if number + 2 < len(marks) - 1:
            points_at_one(number + 2)
    for load in loads[5:]:
        load.wait()

    def run_one(step, total):
        for i in range(8):
            at = step * 8 + i
            total = total + products_one[targets_s[0, at]]
            sums_one[at + 1] = total
        return total

    with jax.named_scope("run_one"):
        sums_one[0] = jnp.zeros(sums_one.shape[1:], jnp.float32)
        lax.fori_loop(0, slots // 8, run_one, jnp.zeros(sums_one.shape[1:], jnp.float32))

    def block_sum(sums, pointers, block):
        return sums[pointers[block + 1]] - sums[pointers[block]]

    def partials(sums, pointers, partial, piece, first, size, more=None):
        per_piece = partial.shape[1]
        step_size = min(size, 8)

        def some(step, carry):
            for i in range(step_size):
                at = first + step * step_size + i
                total = block_sum(sums, pointers, piece * per_piece + at)
                if more is not None:
                    total = total + more[at].astype(jnp.float32)
                partial[piece, at] = total.astype(partial.dtype)
            return carry

        lax.fori_loop(0, size // step_size, some, 0)

    def along(first, last):
        for far in range(first, last, 1 if last > first else -1):
            for sign in (1, -1):
                other = row + sign * far
                yield far, sign, (other >= 0) & (other < rows), other

    end = rows - 1
    chunks = sum_one_sem.shape[1]
    share = partial_one.shape[1] // sum(SPLIT)
    starts = [sum(SPLIT[:h]) * share for h in range(chunks)]
    sizes = [part * share for part in SPLIT]
    parts = [pl.ds(start, size) for start, size in zip(starts, sizes)]

    def sum_copy(h, other):
        return copy_to(
            partial_one.at[other, parts[h]],
            arrived_one.at[row, parts[h]],
            sum_one_sem.at[0, h, other],
            sum_one_sem.at[1, h, row],
            {"row": other},
        )

    def sum_wait(h, other):
        return copy_to(
            partial_one.at[other, parts[h]],
            arrived_one.at[other, parts[h]],
            sum_one_sem.at[0, h, other],
            sum_one_sem.at[1, h, other],
            {"row": other},
        )

    def pass_copy(h, side, other, through):
        return copy_to(
            partial_one.at[other, parts[h]],
            passing.at[side, parts[h]],
            pass_sem.at[0, side, h],
            pass_sem.at[1, side, h],
            {"row": through},
        )

    sides = [(0, 0, 1, end), (1, end, end - 1, 0)]
    def send_ends(h):
        for side, source, through, to in sides:

            @pl.when(row == source)
            def _():
                partials(sums_one, pointers_one, partial_one, to, starts[h], sizes[h])
                pass_copy(h, side, to, through).start()

    def send_sums(h):
        for far, sign, valid, other in along(end - 1, 0):
            direct = valid
            if far == end - 1:
                to = end if sign > 0 else 0
                direct = valid & (other != to)

            @pl.when(direct)
            def _():
                partials(sums_one, pointers_one, partial_one, other, starts[h], sizes[h])
                sum_copy(h, other).start()

    for h in range(chunks + LEAD):
        with jax.named_scope(f"partials#h={h}"):
            if h < chunks:
                send_ends(h)
            if h >= LEAD:
                send_sums(h - LEAD)

    def pass_on(h):
        for side, source, through, to in sides:

            @pl.when(row == through)
            def _():
                pass_copy(h, side, to, through).wait_recv()
                partials(sums_one, pointers_one, partial_one, to, starts[h], sizes[h], passing.at[side])
                sum_copy(h, to).start()

    def own_copy(h, piece, other, out_sem):
        return copy_to(
            group_one.at[piece, parts[h]],
            group_one.at[piece, parts[h]],
            out_sem,
            own_one_sem.at[1, h, piece],
            {"row": other},
        )

    def straight(h):
        return h >= chunks - STRAIGHT

    def own_direct(h, far, other):
        if far == 1 or (far == end and straight(h)):
            return True
        return (other != 0) & (other != end)

    def sum_up(h):
        with jax.named_scope(f"pass#h={h}"):
            pass_on(h)
        for far, sign, valid, other in along(1, rows):
            if far == end:
                continue

            @pl.when(valid)
            def _():
                with jax.named_scope(f"wait_sum#h={h}#far={far}"):
                    sum_wait(h, other).wait_recv()

        with jax.named_scope(f"own#h={h}"):
            base = row * partial_one.shape[1]

            def finish(i):
                at = starts[h] + i
                total = block_sum(sums_one, pointers_one, base + at) + injected_one[at]
                for other in range(rows):
                    comes = (row != other) & ((row - other) * (row - other) < end * end)
                    here = arrived_one[other, at].astype(jnp.float32)
                    total = total + jnp.where(comes, here, 0.0)
                value = total.astype(out_one.dtype)
                out_one[:, at * edge : (at + 1) * edge] = value
                group_one[row, at] = value

            for i in range(sizes[h]):
                finish(i)
            for far, sign, valid, other in along(end, 0):

                @pl.when(valid & own_direct(h, far, other))
                def _():
                    own_copy(h, row, other, own_one_sem.at[0, h, other]).start()

    def points_at_two(first, last):
        with jax.named_scope("points_two"):
            points_groups(
                first,
                last,
                points_two,
                lambda j: group_one[row, j],
                group_one.shape[1],
                min(group_one.shape[1], 32),
                injected_two,
            )

    def onwards(h, valid, other):
        for to, through in ((end, end - 1), (0, 1)):
            gap = (other - to) * (other - to)
            onward = valid & (row == through) & (gap > 1)
            if straight(h):
                onward = onward & (gap < end * end)
            yield to, onward

    def early(h, valid, other):
        passed = False
        for _, onward in onwards(h, valid, other):
            passed = passed | onward
        return passed & (other != 0) & (other != end)

    def receive(h, other, wanted):
        @pl.when(wanted)
        def _():
            own_copy(h, other, row, own_one_sem.at[0, h, other]).wait_recv()

        for to, onward in onwards(h, wanted, other):

            @pl.when(onward)
            def _():
                own_copy(h, other, to, on_sem.at[h, other]).start()

    def receive_early(h):
        for far, sign, valid, other in along(1, rows):
            receive(h, other, early(h, valid, other))

    for h in range(chunks):
        sum_up(h)
        if h > 0:
            receive_early(h - 1)
    receive_early(chunks - 1)

    groups_two = points_two.shape[0]
    for h in range(chunks):
        for far in range(1, rows):
            for sign in (1, -1):
                other = row + sign * far
                valid = (other >= 0) & (other < rows)
                with jax.named_scope(f"wait_own#h={h}#far={far}"):
                    receive(h, other, valid & jnp.logical_not(early(h, valid, other)))
            if h == 0:
                points_at_two(groups_two * (far - 1) // end, groups_two * far // end)

    def drain_one():
        for h in range(chunks):
            for side, source, through, to in sides:

                @pl.when(row == source)
                def _():
                    pass_copy(h, side, to, through).wait_send()

                @pl.when(row == through)
                def _():
                    sum_copy(h, to).wait_send()

            for far, sign, valid, other in along(end - 1, 0):
                direct = valid
                if far == end - 1:
                    to = end if sign > 0 else 0
                    direct = valid & (other != to)

                @pl.when(direct)
                def _():
                    sum_copy(h, other).wait_send()

            for far, sign, valid, other in along(end, 0):

                @pl.when(valid & own_direct(h, far, other))
                def _():
                    own_copy(h, row, other, own_one_sem.at[0, h, other]).wait_send()

                for to, onward in onwards(h, valid, other):

                    @pl.when(onward)
                    def _():
                        own_copy(h, other, to, on_sem.at[h, other]).wait_send()

    def exchange(sums, pointers, partial, arrived, injected, peers, axis, me, sems, group, own_sems, out):
        size = partial.shape[1]
        first, again = [], []
        with jax.named_scope("partials"):
            for k, peer in peers:
                partials(sums, pointers, partial, peer, 0, size)
                first.append(send(partial.at[peer], arrived.at[k - 1], sems, (k - 1,), {axis: peer}))
        own = [block_sum(sums, pointers, me * size + i) + injected[i] for i in range(size)]
        for (k, _), copy in zip(peers, first):
            with jax.named_scope(f"wait_sum#k={k}"):
                copy.wait_recv()
            for i in range(size):
                own[i] = own[i] + arrived[k - 1, i].astype(jnp.float32)
        for i in range(size):
            value = own[i].astype(out.dtype)
            out[:, i * edge : (i + 1) * edge] = value
            if group is not None:
                group[me, i] = value
        if group is not None:
            for k, peer in peers:
                again.append(send(group.at[me], group.at[me], own_sems, (k - 1,), {axis: peer}))
        return first, again

    def restrict(held, columns, group, sums):
        number = held.shape[0]
        batch = min(4 * BATCH, number)
        per_piece = group.shape[1]

        def some(step, total):
            first = step * batch

            def source_of(i):
                column = columns[first + i]
                return group[jnp.right_shift(column, shift_of(per_piece)), jnp.bitwise_and(column, per_piece - 1)]

            found = some_products(held, batch, lambda i: first + i, source_of)
            for i, product in enumerate(found):
                total = total + product
                sums[first + i + 1] = total
            return total

        sums[0] = jnp.zeros(sums.shape[1:], jnp.float32)
        lax.fori_loop(0, number // batch, some, jnp.zeros(sums.shape[1:], jnp.float32))

    with jax.named_scope("restrict_two"):
        restrict(held_two, columns_two, group_one, sums_two)
    sent_two, own_two = exchange(
        sums_two, pointers_two, partial_two, arrived_two, injected_two, far_peers, "col", col, sum_two_sem, group_two,
        own_two_sem, out_two,
    )
    with jax.named_scope("points_three"):
        points_groups(
            0,
            points_three.shape[0],
            points_three,
            lambda j: group_two[col, j],
            group_two.shape[1],
            group_two.shape[1],
            injected_three,
        )
    with jax.named_scope("wait_group_two"):
        for copy in own_two:
            copy.wait_recv()
    with jax.named_scope("restrict_three"):
        restrict(held_three, columns_three, group_two, sums_three)
    sent_three, _ = exchange(
        sums_three, pointers_three, partial_three, arrived_three, injected_three, row_peers, "row", row, sum_three_sem,
        None, None, out_three,
    )
    with jax.named_scope("drain"):
        for copy in asks + answers + sent_two + own_two + sent_three:
            copy.wait_send()
        drain_one()


def tail_kernel(*refs):
    half = len(refs) // 2
    for source, out in zip(refs[:half], refs[half:]):
        out[...] = source[...]


def on_device(
    fine_residual,
    tiles_one,
    pointers_one,
    columns_one,
    points_one,
    tiles_two,
    pointers_two,
    columns_two,
    points_two,
    tiles_three,
    pointers_three,
    columns_three,
    points_three,
):
    vectors = fine_residual.shape[0]
    edge = tiles_one.shape[1]
    rows, cols = lax.axis_size("row"), lax.axis_size("col")
    slots = tiles_one.shape[0]
    per_peer = slots // cols
    low, wide = fine_residual.dtype, jnp.float32
    piece_one = (pointers_one.shape[0] - 1) // rows
    piece_two = (pointers_two.shape[0] - 1) // cols
    piece_three = (pointers_three.shape[0] - 1) // rows
    chunks = len(SPLIT)

    def grouped(points):
        size = points.shape[0] // edge
        group = min(size, 2)
        return points.reshape(size // group, 1, group * edge)

    block = (vectors, edge)
    dma = pltpu.SemaphoreType.DMA
    inputs = [
        (fine_residual, pltpu.VMEM),
        (columns_one.reshape(1, slots), pltpu.VMEM),
        (pointers_one, pltpu.SMEM),
        (pointers_two, pltpu.SMEM),
        (pointers_three, pltpu.SMEM),
        (columns_two, pltpu.SMEM),
        (columns_three, pltpu.SMEM),
        (grouped(points_one), pltpu.VMEM),
        (grouped(points_two), pltpu.VMEM),
        (grouped(points_three), pltpu.VMEM),
        (tiles_one, pltpu.VMEM),
        (tiles_two, pltpu.VMEM),
        (tiles_three, pltpu.VMEM),
    ]
    scratch = [space(array.shape, array.dtype) for array, space in inputs]
    scratch += [
        pltpu.VMEM((1, slots), jnp.int32),
        pltpu.VMEM((1, slots), jnp.int32),
        pltpu.VMEM((1, slots), jnp.int32),
        pltpu.SMEM((1, slots), jnp.int32),
        pltpu.SMEM((1, slots), jnp.int32),
        pltpu.SMEM((cols, 1, slots), jnp.int32),
        pltpu.VMEM((fine_residual.shape[1] // edge,) + block, low),
        pltpu.VMEM((cols - 1, per_peer) + block, low),
        pltpu.VMEM((cols, per_peer) + block, low),
        pltpu.VMEM((slots,) + block, wide),
        pltpu.VMEM((slots + 1,) + block, wide),
        pltpu.VMEM((tiles_two.shape[0] + 1,) + block, wide),
        pltpu.VMEM((tiles_three.shape[0] + 1,) + block, wide),
        pltpu.VMEM((rows, piece_one) + block, low),
        pltpu.VMEM((cols, piece_two) + block, low),
        pltpu.VMEM((rows, piece_three) + block, low),
        pltpu.VMEM((rows, piece_one) + block, low),
        pltpu.VMEM((2, piece_one) + block, low),
        pltpu.VMEM((cols - 1, piece_two) + block, low),
        pltpu.VMEM((rows - 1, piece_three) + block, low),
        pltpu.VMEM((piece_one,) + block, wide),
        pltpu.VMEM((piece_two,) + block, wide),
        pltpu.VMEM((piece_three,) + block, wide),
        pltpu.VMEM((rows, piece_one) + block, low),
        pltpu.VMEM((cols, piece_two) + block, low),
        dma((len(inputs),)),
        dma((3,)),
        dma((2, cols - 1)),
        dma((2, cols - 1)),
        dma((2, chunks, rows)),
        dma((2, 2, chunks)),
        dma((2, chunks, rows)),
        dma((chunks, rows)),
        dma((2, cols - 1)),
        dma((2, cols - 1)),
        dma((2, rows - 1)),
    ]
    shapes = [jax.ShapeDtypeStruct((vectors, piece * edge), low) for piece in (piece_one, piece_two, piece_three)]
    vmem = [pl.BlockSpec(memory_space=pltpu.VMEM)] * 3
    found = pl.pallas_call(
        functools.partial(kernel, (rows, cols)),
        in_specs=[pl.BlockSpec(memory_space=pl.ANY)] * len(inputs),
        out_specs=vmem,
        out_shape=shapes,
        scratch_shapes=scratch,
        compiler_params=pltpu.CompilerParams(
            collective_id=0, has_side_effects=True
        ),
        name="restrict_all",
    )(*[array for array, _ in inputs])
    return pl.pallas_call(
        tail_kernel,
        in_specs=vmem,
        out_specs=vmem,
        out_shape=shapes,
        name="results",
    )(*found)


def solution(mesh):
    placed = (
        P(None, ("row", "col")),
        P(("row", "col"), None, None),
        P(("row", "col")),
        P(("row", "col")),
        P(("col", "row")),
        P(("row", "col"), None, None),
        P(("row", "col")),
        P(("row", "col")),
        P(("row", "col")),
        P(("row", "col"), None, None),
        P(("row", "col")),
        P(("row", "col")),
        P(("col", "row")),
    )
    return jax.shard_map(
        on_device,
        mesh=mesh,
        in_specs=placed,
        out_specs=(P(None, ("col", "row")), P(None, ("row", "col")), P(None, ("col", "row"))),
        check_vma=False,
    )
```
